128 devices in a mesh: slab: 2 (over y_hi), pencil: 64 (over x, y_lo, z, core).
Axes of the slice: x: 4, y: 4 (y_hi: 2, y_lo: 2; y = y_hi * 2 + y_lo), z: 4, core: 2. Of those that a mesh axis runs over, the one named last changes fastest.
Arguments:
- concentration: float32 [512, 512, 256], P('slab', 'pencil'), may hold values from -2 to 2.8
Outputs:
- updated: float32 [512, 512, 256], P('slab', 'pencil')
- mass: float32 [], replicated
The draws below stay inside these ranges and needn't reach their ends.
All inputs are finite; a program needn't handle non-finite values.
Results may differ from the reference program's by a relative error of at most 0.0002.
Values sent between devices are 32-bit elements; how exact they have to be, the bound alone decides.
A program may use at most 128 MiB of HBM per device.

```python
import math
import jax
import jax.numpy as jnp

NX = 512
NY = 512
NZ = 256


def draw_concentration(key, part):
    noise_key = jax.random.fold_in(key, 11)
    phase_key = jax.random.fold_in(key, 23)
    first = jnp.arange(NX, dtype=jnp.float32)[:, None, None] / NX
    second = jnp.arange(NY, dtype=jnp.float32)[None, :, None] / NY
    third = jnp.arange(NZ, dtype=jnp.float32)[None, None, :] / NZ
    profile = 0.1 + 0.2 * first + 0.5 * second
    parity = jnp.arange(NX, dtype=jnp.int32) % 2
    alternate = jnp.where(parity == 0, 1.0, -1.0).astype(jnp.float32)[:, None, None]
    phases = jax.random.uniform(phase_key, (4,), jnp.float32, 0.0, 2.0 * math.pi)
    envelope = 0.75 + 0.125 * jnp.sin(2.0 * math.pi * second + phases[2]) + 0.125 * jnp.cos(2.0 * math.pi * third + phases[3])
    noise = 0.2 * jnp.clip(jax.random.normal(noise_key, (NX, NY, NZ), jnp.float32), -2.5, 2.5)
    return (profile + 1.5 * envelope * alternate + noise).astype(jnp.float32)


def setup_inputs(seed: int = 0) -> dict:
    streams_of = jax.random.split(jax.random.key(seed), 2)
    return {
        "concentration": draw_concentration(jax.random.fold_in(streams_of[1], 71), 0),
    }


time_step = 1.0
stiffness = 1.0


def wavenumber(length):
    index = jnp.arange(length, dtype=jnp.int32)
    signed = jnp.where(index < length // 2, index, index - length)
    return (2.0 * math.pi / length) * signed.astype(jnp.float32)


def reference(concentration):
    cube = concentration * concentration * concentration
    conc_hat = jnp.fft.fftn(concentration)
    cube_hat = jnp.fft.fftn(cube)
    wave_first = wavenumber(NX)
    wave_second = wavenumber(NY)
    wave_third = wavenumber(NZ)
    wave_square = wave_first[:, None, None] ** 2 + wave_second[None, :, None] ** 2 + wave_third[None, None, :] ** 2
    keep = jnp.where(jnp.arange(NZ, dtype=jnp.int32) == NZ // 2, 0.0, 1.0)[None, None, :]
    divisor = 1.0 + time_step * stiffness * wave_square * wave_square
    retain = keep * (1.0 + time_step * wave_square) / divisor
    forcing = keep * (time_step * wave_square) / divisor
    next_hat = retain * conc_hat - forcing * cube_hat
    updated = jnp.real(jnp.fft.ifftn(next_hat)).astype(concentration.dtype)
    mass = jnp.sum(concentration) / (NX * NY * NZ)
    return updated, mass
```

```python
import functools
import math

import jax
import jax.numpy as jnp
import numpy as np
from jax import lax
from jax.experimental import pallas as pl
from jax.experimental.pallas import tpu as pltpu
from jax.sharding import PartitionSpec as P

NX = 512
NY = 512
NZ = 256
KEPT = NZ // 2
DEVICES = 128
ROWS = 256
COLS = 8
HALF = ROWS // 2
TOTAL = NX * NY * NZ

time_step = 1.0
stiffness = 1.0

MESH = pl.DeviceIdType.MESH
f32 = jnp.float32
bf16 = jnp.bfloat16


def split_table(table):
    high = table.astype(np.float32).astype(bf16)
    low = (table - high.astype(np.float64)).astype(np.float32).astype(bf16)
    return np.stack([high, low])


def depth_tables():
    k = np.arange(KEPT)[:, None]
    n = np.arange(NZ)[None, :]
    angle = 2.0 * np.pi * (k * n % NZ) / NZ
    forward = np.concatenate([np.cos(angle), -np.sin(angle)], axis=0)
    weight = np.where(k == 0, 1.0, 2.0) / TOTAL
    inverse = np.stack([weight * np.cos(angle), -weight * np.sin(angle)], axis=1)
    return split_table(forward), split_table(inverse.reshape(NZ, NZ))


def plane_tables():
    c = np.arange(128)[:, None]
    b = np.arange(128)[None, :]
    out = []
    for d in range(4):
        angle = 2.0 * np.pi * (b * (4 * c + d) % 512) / 512
        cos, sin = np.cos(angle), np.sin(angle)
        out.append(np.block([[cos, sin], [-sin, cos]]))
    full = np.stack(out)
    return split_table(full), split_table(full.transpose(0, 2, 1))


def parts(value):
    high = value.astype(bf16)
    return high, (value - high.astype(f32)).astype(bf16)


def product(left, right, dims):
    dot = functools.partial(
        lax.dot_general, dimension_numbers=(dims, ((), ())), preferred_element_type=f32
    )
    return dot(left[0], right[0]) + (dot(left[0], right[1]) + dot(left[1], right[0]))


def spread(xr, xi):
    sr, si = xr[0] + xr[2], xi[0] + xi[2]
    tr, ti = xr[1] + xr[3], xi[1] + xi[3]
    pr, pi = xr[0] - xr[2], xi[0] - xi[2]
    qr, qi = xr[1] - xr[3], xi[1] - xi[3]
    return (
        (sr + tr, si + ti),
        (pr + qi, pi - qr),
        (sr - tr, si - ti),
        (pr - qi, pi + qr),
    )


def gather(vr, vi):
    sr, si = vr[0] + vr[2], vi[0] + vi[2]
    tr, ti = vr[1] + vr[3], vi[1] + vi[3]
    pr, pi = vr[0] - vr[2], vi[0] - vi[2]
    qr, qi = vr[1] - vr[3], vi[1] - vi[3]
    return (
        (sr + tr, si + ti),
        (pr - qi, pi + qr),
        (sr - tr, si - ti),
        (pr + qi, pi - qr),
    )


def shifted(me, step):
    y = (me // 64 * 2 + me // 8 % 2 + step // 64 * 2 + step // 8 % 2) % 4
    x = (me // 16 + step // 16) % 4
    z = (me // 2 + step // 2) % 4
    core = (me + step) % 2
    return y // 2 * 64 + x * 16 + y % 2 * 8 + z * 2 + core


def wave(index):
    signed = jnp.where(index < 256, index, index - 512)
    return (2.0 * math.pi / 512) * signed.astype(f32)


def kernel(
    conc_hbm, zf_hbm, zi_hbm, pf_hbm, pt_hbm,
    out_hbm, mass_ref,
    conc, zf, zi, pf, pt, send_c, send_q, plane, back, got, out, retain, forcing,
    load_sem, out_sem, local_sem, send_sem, recv_sem,
):
    slab = lax.axis_index("slab")
    pencil = lax.axis_index("pencil")
    me = slab * 64 + pencil

    barrier = pltpu.get_barrier_semaphore()

    def greet(step, carry):
        to = shifted(me, step)
        pl.semaphore_signal(
            barrier, inc=1, device_id=(to // 64, to % 64), device_id_type=MESH
        )
        return carry

    loads = [
        pltpu.make_async_copy(src, dst, load_sem.at[i])
        for i, (src, dst) in enumerate(
            [
                (conc_hbm.at[:, 0:128], conc.at[0]),
                (conc_hbm.at[:, 128:256], conc.at[1]),
                (zf_hbm, zf),
                (pf_hbm, pf),
                (pt_hbm, pt),
                (zi_hbm, zi),
            ]
        )
    ]
    for load in loads:
        load.start()
    lax.fori_loop(1, DEVICES, greet, 0)
    for load in loads:
        load.wait()

    def depth_forward(cubed, sends):
        def body(y, carry):
            value = jnp.concatenate(
                [conc[i, pl.ds(y, ROWS, stride=COLS), :] for i in range(2)], axis=1
            )
            if cubed:
                value = value * value * value
            result = product((zf[0], zf[1]), parts(value), ((1,), (1,)))
            for i in range(2):
                for h in range(2):
                    sends[h, pl.ds(i * COLS + y, KEPT, stride=2 * COLS), :] = result[
                        i * KEPT : (i + 1) * KEPT, h * HALF : (h + 1) * HALF
                    ]
            return carry

        lax.fori_loop(0, COLS, body, 0)

    def forward_block(sends, field, h, to):
        return (
            sends.at[h, pl.ds(pl.multiple_of(to * 16, 16), 16), :].reshape(2, 8, 128),
            plane.at[
                2 * field : 2 * field + 2,
                pl.ds(pl.multiple_of(pencil * COLS, COLS), COLS),
                pl.ds(pl.multiple_of(slab * ROWS + h * HALF, HALF), HALF),
            ],
        )

    def backward_block(h, to):
        return (
            back.at[
                :,
                pl.ds(pl.multiple_of(to % 64 * COLS, COLS), COLS),
                pl.ds(pl.multiple_of(to // 64 * ROWS + h * HALF, HALF), HALF),
            ],
            got.at[h, pl.ds(pl.multiple_of(me * 16, 16), 16), :].reshape(2, 8, 128),
        )

    def exchange(block, stage):
        src, dst = block(me)
        pltpu.make_async_copy(src, dst, local_sem.at[stage]).start()

        def send(turn, carry):
            to = shifted(me, turn * 21 % 128)
            src, dst = block(to)
            pltpu.make_async_remote_copy(
                src_ref=src,
                dst_ref=dst,
                send_sem=send_sem.at[stage],
                recv_sem=recv_sem.at[stage],
                device_id=(to // 64, to % 64),
                device_id_type=MESH,
            ).start()
            return carry

        lax.fori_loop(1, DEVICES, send, 0)

    def arrived(block, stage):
        src, dst = block(me)
        pltpu.make_async_copy(src, dst, local_sem.at[stage]).wait()
        rows = pl.ds(0, 16 * (DEVICES - 1))
        everything = pltpu.make_async_remote_copy(
            src_ref=got.at[0, rows, :],
            dst_ref=got.at[0, rows, :],
            send_sem=send_sem.at[stage],
            recv_sem=recv_sem.at[stage],
            device_id=(slab, pencil),
            device_id_type=MESH,
        )
        everything.wait()

    def second_forward(field):
        def body(i, carry):
            lanes = pl.ds(pl.multiple_of(i * 256, 256), 256)
            xr = [plane[2 * field, a * 128 : (a + 1) * 128, lanes] for a in range(4)]
            xi = [plane[2 * field + 1, a * 128 : (a + 1) * 128, lanes] for a in range(4)]
            for d, (ur, ui) in enumerate(spread(xr, xi)):
                result = product(
                    (pf[0, d], pf[1, d]), parts(jnp.concatenate([ur, ui], axis=0)), ((1,), (0,))
                )
                plane[2 * field, d * 128 : (d + 1) * 128, lanes] = result[:128]
                plane[2 * field + 1, d * 128 : (d + 1) * 128, lanes] = result[128:]
            return carry

        lax.fori_loop(0, 2, body, 0)

    def first_forward(field, rows):
        xr = [plane[2 * field, rows, a * 128 : (a + 1) * 128] for a in range(4)]
        xi = [plane[2 * field + 1, rows, a * 128 : (a + 1) * 128] for a in range(4)]
        return [
            product(parts(jnp.concatenate([ur, ui], axis=1)), (pt[0, d], pt[1, d]), ((1,), (0,)))
            for d, (ur, ui) in enumerate(spread(xr, xi))
        ]

    def row_block(i):
        return pl.ds(pl.multiple_of(i * 128, 128), 128)

    def first_forward_conc():
        def body(i, carry):
            rows = row_block(i)
            for d, result in enumerate(first_forward(0, rows)):
                plane[0, rows, d * 128 : (d + 1) * 128] = result[:, :128]
                plane[1, rows, d * 128 : (d + 1) * 128] = result[:, 128:]
            return carry

        lax.fori_loop(0, 4, body, 0)

    def multipliers():
        third = wave(me) * (512 // NZ)

        def body(i, carry):
            rows = row_block(i)
            row = lax.broadcasted_iota(jnp.int32, (128, 512), 0)
            lane = lax.broadcasted_iota(jnp.int32, (128, 512), 1)
            second = wave(row * 4 + i)
            first = wave(lane % 128 * 4 + lane // 128)
            square = first * first + second * second + third * third
            divisor = 1.0 + time_step * stiffness * square * square
            retain[rows, :] = (1.0 + time_step * square) / divisor
            forcing[rows, :] = (time_step * square) / divisor
            return carry

        lax.fori_loop(0, 4, body, 0)

    def combine_and_first_inverse():
        def body(i, carry):
            rows = row_block(i)
            vr, vi = [], []
            for d, cube in enumerate(first_forward(1, rows)):
                lanes = slice(d * 128, (d + 1) * 128)
                keep, force = retain[rows, lanes], forcing[rows, lanes]
                next_real = keep * plane[0, rows, lanes] - force * cube[:, :128]
                next_imag = keep * plane[1, rows, lanes] - force * cube[:, 128:]
                result = product(
                    parts(jnp.concatenate([next_real, next_imag], axis=1)),
                    (pf[0, d], pf[1, d]),
                    ((1,), (0,)),
                )
                vr.append(result[:, :128])
                vi.append(result[:, 128:])
            for a, (xr, xi) in enumerate(gather(vr, vi)):
                plane[2, rows, a * 128 : (a + 1) * 128] = xr
                plane[3, rows, a * 128 : (a + 1) * 128] = xi
            return carry

        lax.fori_loop(0, 4, body, 0)

    def second_inverse(h, mass):
        def body(i, carry):
            lanes = pl.ds(pl.multiple_of(i * ROWS + h * HALF, HALF), HALF)
            vr, vi = [], []
            for d in range(4):
                block = slice(d * 128, (d + 1) * 128)
                result = product(
                    (pt[0, d], pt[1, d]),
                    parts(jnp.concatenate([plane[2, block, lanes], plane[3, block, lanes]], axis=0)),
                    ((1,), (0,)),
                )
                vr.append(result[:128])
                vi.append(result[128:])
            for a, (xr, xi) in enumerate(gather(vr, vi)):
                block = slice(a * 128, (a + 1) * 128)
                back[0, block, lanes] = xr
                back[1, block, lanes] = jnp.where(me == 0, mass, xi)
            return carry

        lax.fori_loop(0, 2, body, 0)

    def depth_inverse(h):
        def body(y, carry):
            value = got[h, pl.ds(y, NZ, stride=COLS), :]
            result = product(parts(value), (zi[0], zi[1]), ((0,), (0,)))
            for i in range(2):
                out[i, pl.ds(h * HALF * COLS + y, HALF, stride=COLS), :] = result[
                    :, i * 128 : (i + 1) * 128
                ]
            return carry

        lax.fori_loop(0, COLS, body, 0)

    depth_forward(False, send_c)
    pl.semaphore_wait(barrier, DEVICES - 1)
    for h in range(2):
        exchange(functools.partial(forward_block, send_c, 0, h), h)
    depth_forward(True, send_q)
    for h in range(2):
        exchange(functools.partial(forward_block, send_q, 1, h), 2 + h)
    multipliers()
    for h in range(2):
        arrived(functools.partial(forward_block, send_c, 0, h), h)
    second_forward(0)
    first_forward_conc()
    mass = jnp.broadcast_to(plane[0, 0:1, 0:1], (128, 128)) * (1.0 / TOTAL)
    for h in range(2):
        arrived(functools.partial(forward_block, send_q, 1, h), 2 + h)
    second_forward(1)
    combine_and_first_inverse()
    for h in range(2):
        second_inverse(h, mass)
        exchange(functools.partial(backward_block, h), 4 + h)
    outs = []
    for h in range(2):
        arrived(functools.partial(backward_block, h), 4 + h)
        depth_inverse(h)
        rows = pl.ds(h * HALF * COLS, HALF * COLS)
        for i in range(2):
            outs.append(
                pltpu.make_async_copy(
                    out.at[i, rows, :],
                    out_hbm.at[rows, i * 128 : (i + 1) * 128],
                    out_sem.at[h, i],
                )
            )
            outs[-1].start()
    mass_ref[...] = got[0, 8:16, :]
    for copy in outs:
        copy.wait()


def local(concentration):
    zf, zi = depth_tables()
    pf, pt = plane_tables()
    anywhere = pl.BlockSpec(memory_space=pl.ANY)
    updated, mass = pl.pallas_call(
        kernel,
        out_shape=(
            jax.ShapeDtypeStruct((ROWS * COLS, NZ), f32),
            jax.ShapeDtypeStruct((8, 128), f32),
        ),
        in_specs=[anywhere] * 5,
        out_specs=(anywhere, pl.BlockSpec(memory_space=pltpu.VMEM)),
        scratch_shapes=[
            pltpu.VMEM((2, ROWS * COLS, 128), f32),
            pltpu.VMEM(zf.shape, bf16),
            pltpu.VMEM(zi.shape, bf16),
            pltpu.VMEM(pf.shape, bf16),
            pltpu.VMEM(pt.shape, bf16),
            pltpu.VMEM((2, KEPT * 16, HALF), f32),
            pltpu.VMEM((2, KEPT * 16, HALF), f32),
            pltpu.VMEM((4, NY, NX), f32),
            pltpu.VMEM((2, NY, NX), f32),
            pltpu.VMEM((2, KEPT * 16, HALF), f32),
            pltpu.VMEM((2, ROWS * COLS, 128), f32),
            pltpu.VMEM((NY, NX), f32),
            pltpu.VMEM((NY, NX), f32),
            pltpu.SemaphoreType.DMA((6,)),
            pltpu.SemaphoreType.DMA((2, 2)),
            pltpu.SemaphoreType.DMA((6,)),
            pltpu.SemaphoreType.DMA((6,)),
            pltpu.SemaphoreType.DMA((6,)),
        ],
        compiler_params=pltpu.CompilerParams(
            collective_id=0, has_side_effects=True, vmem_limit_bytes=56 * 2**20
        ),
        name="cahn_hilliard_step",
    )(
        concentration.reshape(ROWS * COLS, NZ),
        jnp.asarray(zf), jnp.asarray(zi), jnp.asarray(pf), jnp.asarray(pt),
    )
    return updated.reshape(ROWS, COLS, NZ), mass[0, 0]


def solution(mesh):
    return jax.shard_map(
        local,
        mesh=mesh,
        in_specs=(P("slab", "pencil", None),),
        out_specs=(P("slab", "pencil", None), P()),
        check_vma=False,
    )
```

```python
import functools
import math

import jax
import jax.numpy as jnp
import numpy as np
from jax import lax
from jax.experimental import pallas as pl
from jax.experimental.pallas import tpu as pltpu
from jax.sharding import PartitionSpec as P

NX = 512
NY = 512
NZ = 256
KEPT = NZ // 2
DEVICES = 128
ROWS = 256
COLS = 8
HALF = ROWS // 2
TOTAL = NX * NY * NZ

time_step = 1.0
stiffness = 1.0

MESH = pl.DeviceIdType.MESH
f32 = jnp.float32
bf16 = jnp.bfloat16


def split_table(table):
    high = table.astype(np.float32).astype(bf16)
    low = (table - high.astype(np.float64)).astype(np.float32).astype(bf16)
    return np.stack([high, low])


def depth_tables():
    k = np.arange(KEPT)[:, None]
    n = np.arange(NZ)[None, :]
    angle = 2.0 * np.pi * (k * n % NZ) / NZ
    forward = np.concatenate([np.cos(angle), -np.sin(angle)], axis=0)
    weight = np.where(k == 0, 1.0, 2.0) / TOTAL
    inverse = np.stack([weight * np.cos(angle), -weight * np.sin(angle)], axis=1)
    return split_table(forward), split_table(inverse.reshape(NZ, NZ))


def plane_tables():
    c = np.arange(128)[:, None]
    b = np.arange(128)[None, :]
    out = []
    for d in range(4):
        angle = 2.0 * np.pi * (b * (4 * c + d) % 512) / 512
        cos, sin = np.cos(angle), np.sin(angle)
        out.append(np.block([[cos, sin], [-sin, cos]]))
    full = np.stack(out)
    return split_table(full), split_table(full.transpose(0, 2, 1))


def parts(value):
    high = value.astype(bf16)
    return high, (value - high.astype(f32)).astype(bf16)


def product(left, right, dims):
    dot = functools.partial(
        lax.dot_general, dimension_numbers=(dims, ((), ())), preferred_element_type=f32
    )
    return dot(left[0], right[0]) + (dot(left[0], right[1]) + dot(left[1], right[0]))


def spread(xr, xi):
    sr, si = xr[0] + xr[2], xi[0] + xi[2]
    tr, ti = xr[1] + xr[3], xi[1] + xi[3]
    pr, pi = xr[0] - xr[2], xi[0] - xi[2]
    qr, qi = xr[1] - xr[3], xi[1] - xi[3]
    return (
        (sr + tr, si + ti),
        (pr + qi, pi - qr),
        (sr - tr, si - ti),
        (pr - qi, pi + qr),
    )


def gather(vr, vi):
    sr, si = vr[0] + vr[2], vi[0] + vi[2]
    tr, ti = vr[1] + vr[3], vi[1] + vi[3]
    pr, pi = vr[0] - vr[2], vi[0] - vi[2]
    qr, qi = vr[1] - vr[3], vi[1] - vi[3]
    return (
        (sr + tr, si + ti),
        (pr - qi, pi + qr),
        (sr - tr, si - ti),
        (pr + qi, pi - qr),
    )


def wave(index):
    signed = jnp.where(index < 256, index, index - 512)
    return (2.0 * math.pi / 512) * signed.astype(f32)


def kernel(
    conc_hbm, zf_hbm, zi_hbm, pf_hbm, pt_hbm,
    out_hbm, mass_ref,
    conc, zf, zi, pf, pt, send_c, send_q, plane, back, got, out, retain, forcing,
    load_sem, out_sem, local_sem, send_sem, recv_sem,
):
    slab = lax.axis_index("slab")
    pencil = lax.axis_index("pencil")
    me = slab * 64 + pencil

    barrier = pltpu.get_barrier_semaphore()

    def greet(step, carry):
        to = lax.rem(me + step, DEVICES)
        pl.semaphore_signal(
            barrier,
            inc=1,
            device_id=(lax.div(to, 64), lax.rem(to, 64)),
            device_id_type=MESH,
        )
        return carry

    loads = [
        pltpu.make_async_copy(src, dst, load_sem.at[i])
        for i, (src, dst) in enumerate(
            [
                (conc_hbm.at[:, 0:128], conc.at[0]),
                (conc_hbm.at[:, 128:256], conc.at[1]),
                (zf_hbm, zf),
                (pf_hbm, pf),
                (pt_hbm, pt),
                (zi_hbm, zi),
            ]
        )
    ]
    for load in loads:
        load.start()
    lax.fori_loop(1, DEVICES, greet, 0)
    for load in loads:
        load.wait()

    def depth_forward(cubed, sends, h):
        def body(j, carry):
            value = jnp.concatenate(
                [
                    jnp.concatenate(
                        [
                            conc[i, pl.ds(h * HALF * COLS + 2 * j + e, HALF, stride=COLS), :]
                            for i in range(2)
                        ],
                        axis=1,
                    )
                    for e in range(2)
                ],
                axis=0,
            )
            if cubed:
                value = value * value * value
            result = product((zf[0], zf[1]), parts(value), ((1,), (1,)))
            for i in range(2):
                for e in range(2):
                    sends[h, pl.ds(i * COLS + 2 * j + e, KEPT, stride=2 * COLS), :] = result[
                        i * KEPT : (i + 1) * KEPT, e * HALF : (e + 1) * HALF
                    ]
            return carry

        lax.fori_loop(0, COLS // 2, body, 0)

    def forward_block(sends, field, h, to_slab, to_pencil):
        return (
            sends.at[
                h, pl.ds(pl.multiple_of(to_slab * 1024 + to_pencil * 16, 16), 16), :
            ].reshape(2, 8, 128),
            plane.at[
                2 * field : 2 * field + 2,
                pl.ds(pl.multiple_of(pencil * COLS, COLS), COLS),
                pl.ds(pl.multiple_of(slab * ROWS + h * HALF, HALF), HALF),
            ],
        )

    def backward_block(h, to_slab, to_pencil):
        return (
            back.at[
                :,
                pl.ds(pl.multiple_of(to_pencil * COLS, COLS), COLS),
                pl.ds(pl.multiple_of(to_slab * ROWS + h * HALF, HALF), HALF),
            ],
            got.at[h, pl.ds(pl.multiple_of(me * 16, 16), 16), :].reshape(2, 8, 128),
        )

    def exchange(block, stage):
        src, dst = block(slab, pencil)
        pltpu.make_async_copy(src, dst, local_sem.at[stage]).start()

        def send(to_slab, to_pencil):
            src, dst = block(to_slab, to_pencil)
            pltpu.make_async_remote_copy(
                src_ref=src,
                dst_ref=dst,
                send_sem=send_sem.at[stage],
                recv_sem=recv_sem.at[stage],
                device_id=(to_slab, to_pencil),
                device_id_type=MESH,
            ).start()

        def pair(turn, carry):
            to_pencil = lax.rem(pencil + 11 * turn, 64)
            send(slab, to_pencil)
            send(1 - slab, to_pencil)
            return carry

        send(1 - slab, pencil)
        lax.fori_loop(1, 64, pair, 0)

    def arrived(block, stage):
        src, dst = block(slab, pencil)
        pltpu.make_async_copy(src, dst, local_sem.at[stage]).wait()
        rows = pl.ds(0, 16 * (DEVICES - 1))
        everything = pltpu.make_async_remote_copy(
            src_ref=got.at[0, rows, :],
            dst_ref=got.at[0, rows, :],
            send_sem=send_sem.at[stage],
            recv_sem=recv_sem.at[stage],
            device_id=(slab, pencil),
            device_id_type=MESH,
        )
        everything.wait()

    def lane_halves(h):
        return [slice(i * ROWS + h * HALF, i * ROWS + (h + 1) * HALF) for i in range(2)]

    def both(index, rows, h):
        return jnp.concatenate([plane[index, rows, lanes] for lanes in lane_halves(h)], axis=1)

    def second_forward(field, h):
        quarters = [slice(a * 128, (a + 1) * 128) for a in range(4)]
        xr = [both(2 * field, rows, h) for rows in quarters]
        xi = [both(2 * field + 1, rows, h) for rows in quarters]
        for d, (ur, ui) in enumerate(spread(xr, xi)):
            result = product(
                (pf[0, d], pf[1, d]), parts(jnp.concatenate([ur, ui], axis=0)), ((1,), (0,))
            )
            for i, lanes in enumerate(lane_halves(h)):
                half = slice(i * HALF, (i + 1) * HALF)
                plane[2 * field, quarters[d], lanes] = result[:128, half]
                plane[2 * field + 1, quarters[d], lanes] = result[128:, half]

    def first_forward(field, rows):
        xr = [plane[2 * field, rows, a * 128 : (a + 1) * 128] for a in range(4)]
        xi = [plane[2 * field + 1, rows, a * 128 : (a + 1) * 128] for a in range(4)]
        return [
            product(parts(jnp.concatenate([ur, ui], axis=1)), (pt[0, d], pt[1, d]), ((1,), (0,)))
            for d, (ur, ui) in enumerate(spread(xr, xi))
        ]

    def row_block(i):
        return pl.ds(pl.multiple_of(i * 128, 128), 128)

    def first_forward_conc():
        def body(i, carry):
            rows = row_block(i)
            for d, result in enumerate(first_forward(0, rows)):
                plane[0, rows, d * 128 : (d + 1) * 128] = result[:, :128]
                plane[1, rows, d * 128 : (d + 1) * 128] = result[:, 128:]
            return carry

        lax.fori_loop(0, 4, body, 0)

    def multipliers():
        third = wave(me) * (512 // NZ)

        def body(i, carry):
            rows = row_block(i)
            row = lax.broadcasted_iota(jnp.int32, (128, 512), 0)
            lane = lax.broadcasted_iota(jnp.int32, (128, 512), 1)
            second = wave(row * 4 + i)
            first = wave(lane % 128 * 4 + lane // 128)
            square = first * first + second * second + third * third
            divisor = 1.0 + time_step * stiffness * square * square
            retain[rows, :] = (1.0 + time_step * square) / divisor
            forcing[rows, :] = (time_step * square) / divisor
            return carry

        lax.fori_loop(0, 4, body, 0)

    def combine_and_first_inverse():
        def body(i, carry):
            rows = row_block(i)
            vr, vi = [], []
            for d, cube in enumerate(first_forward(1, rows)):
                lanes = slice(d * 128, (d + 1) * 128)
                keep, force = retain[rows, lanes], forcing[rows, lanes]
                next_real = keep * plane[0, rows, lanes] - force * cube[:, :128]
                next_imag = keep * plane[1, rows, lanes] - force * cube[:, 128:]
                result = product(
                    parts(jnp.concatenate([next_real, next_imag], axis=1)),
                    (pf[0, d], pf[1, d]),
                    ((1,), (0,)),
                )
                vr.append(result[:, :128])
                vi.append(result[:, 128:])
            for a, (xr, xi) in enumerate(gather(vr, vi)):
                plane[2, rows, a * 128 : (a + 1) * 128] = xr
                plane[3, rows, a * 128 : (a + 1) * 128] = xi
            return carry

        lax.fori_loop(0, 4, body, 0)

    def second_inverse(h, mass):
        quarters = [slice(a * 128, (a + 1) * 128) for a in range(4)]
        vr, vi = [], []
        for d in range(4):
            value = jnp.concatenate([both(2, quarters[d], h), both(3, quarters[d], h)], axis=0)
            result = product((pt[0, d], pt[1, d]), parts(value), ((1,), (0,)))
            vr.append(result[:128])
            vi.append(result[128:])
        for a, (xr, xi) in enumerate(gather(vr, vi)):
            xi = jnp.where(me == 0, mass, xi)
            for i, lanes in enumerate(lane_halves(h)):
                half = slice(i * HALF, (i + 1) * HALF)
                back[0, quarters[a], lanes] = xr[:, half]
                back[1, quarters[a], lanes] = xi[:, half]

    def depth_inverse(h):
        def body(j, carry):
            value = jnp.concatenate(
                [got[h, pl.ds(2 * j + e, NZ, stride=COLS), :] for e in range(2)], axis=1
            )
            result = product(parts(value), (zi[0], zi[1]), ((0,), (0,)))
            for e in range(2):
                for i in range(2):
                    out[i, pl.ds(h * HALF * COLS + 2 * j + e, HALF, stride=COLS), :] = result[
                        e * HALF : (e + 1) * HALF, i * 128 : (i + 1) * 128
                    ]
            return carry

        lax.fori_loop(0, COLS // 2, body, 0)

    depth_forward(False, send_c, 0)
    pl.semaphore_wait(barrier, DEVICES - 1)
    exchange(functools.partial(forward_block, send_c, 0, 0), 0)
    depth_forward(False, send_c, 1)
    exchange(functools.partial(forward_block, send_c, 0, 1), 1)
    for h in range(2):
        depth_forward(True, send_q, h)
        exchange(functools.partial(forward_block, send_q, 1, h), 2 + h)
    multipliers()
    for h in range(2):
        arrived(functools.partial(forward_block, send_c, 0, h), h)
        second_forward(0, h)
    first_forward_conc()
    mass = jnp.broadcast_to(plane[0, 0:1, 0:1], (128, 256)) * (1.0 / TOTAL)
    for h in range(2):
        arrived(functools.partial(forward_block, send_q, 1, h), 2 + h)
        second_forward(1, h)
    combine_and_first_inverse()
    for h in range(2):
        second_inverse(h, mass)
        exchange(functools.partial(backward_block, h), 4 + h)
    outs = []
    for h in range(2):
        arrived(functools.partial(backward_block, h), 4 + h)
        depth_inverse(h)
        rows = pl.ds(h * HALF * COLS, HALF * COLS)
        for i in range(2):
            outs.append(
                pltpu.make_async_copy(
                    out.at[i, rows, :],
                    out_hbm.at[rows, i * 128 : (i + 1) * 128],
                    out_sem.at[h, i],
                )
            )
            outs[-1].start()
    mass_ref[...] = got[0, 8:16, :]
    for copy in outs:
        copy.wait()


def local(concentration):
    zf, zi = depth_tables()
    pf, pt = plane_tables()
    anywhere = pl.BlockSpec(memory_space=pl.ANY)
    updated, mass = pl.pallas_call(
        kernel,
        out_shape=(
            jax.ShapeDtypeStruct((ROWS * COLS, NZ), f32),
            jax.ShapeDtypeStruct((8, 128), f32),
        ),
        in_specs=[anywhere] * 5,
        out_specs=(anywhere, pl.BlockSpec(memory_space=pltpu.VMEM)),
        scratch_shapes=[
            pltpu.VMEM((2, ROWS * COLS, 128), f32),
            pltpu.VMEM(zf.shape, bf16),
            pltpu.VMEM(zi.shape, bf16),
            pltpu.VMEM(pf.shape, bf16),
            pltpu.VMEM(pt.shape, bf16),
            pltpu.VMEM((2, KEPT * 16, HALF), f32),
            pltpu.VMEM((2, KEPT * 16, HALF), f32),
            pltpu.VMEM((4, NY, NX), f32),
            pltpu.VMEM((2, NY, NX), f32),
            pltpu.VMEM((2, KEPT * 16, HALF), f32),
            pltpu.VMEM((2, ROWS * COLS, 128), f32),
            pltpu.VMEM((NY, NX), f32),
            pltpu.VMEM((NY, NX), f32),
            pltpu.SemaphoreType.DMA((6,)),
            pltpu.SemaphoreType.DMA((2, 2)),
            pltpu.SemaphoreType.DMA((6,)),
            pltpu.SemaphoreType.DMA((6,)),
            pltpu.SemaphoreType.DMA((6,)),
        ],
        compiler_params=pltpu.CompilerParams(
            collective_id=0, has_side_effects=True, vmem_limit_bytes=56 * 2**20
        ),
        name="cahn_hilliard_step",
    )(
        concentration.reshape(ROWS * COLS, NZ),
        jnp.asarray(zf), jnp.asarray(zi), jnp.asarray(pf), jnp.asarray(pt),
    )
    return updated.reshape(ROWS, COLS, NZ), mass[0, 0]


def solution(mesh):
    return jax.shard_map(
        local,
        mesh=mesh,
        in_specs=(P("slab", "pencil", None),),
        out_specs=(P("slab", "pencil", None), P()),
        check_vma=False,
    )
```

```python
import functools
import math

import jax
import jax.numpy as jnp
import numpy as np
from jax import lax
from jax.experimental import pallas as pl
from jax.experimental.pallas import tpu as pltpu
from jax.sharding import PartitionSpec as P

NX = 512
NY = 512
NZ = 256
KEPT = NZ // 2
DEVICES = 128
ROWS = 256
COLS = 8
HALF = ROWS // 2
TOTAL = NX * NY * NZ
FIRST = 1

time_step = 1.0
stiffness = 1.0

MESH = pl.DeviceIdType.MESH
f32 = jnp.float32
bf16 = jnp.bfloat16


def all_tables():
    full = np.concatenate([depth_tables(), *plane_tables()])
    high = full.astype(np.float32).astype(bf16)
    low = (full - high.astype(np.float64)).astype(np.float32).astype(bf16)
    return np.stack([high, low], axis=1).reshape(20, 256, 256)


def depth_tables():
    k = np.arange(KEPT)[:, None]
    n = np.arange(NZ)[None, :]
    angle = 2.0 * np.pi * (k * n % NZ) / NZ
    forward = np.concatenate([np.cos(angle), -np.sin(angle)], axis=0)
    weight = np.where(k == 0, 1.0, 2.0) / TOTAL
    inverse = np.stack([weight * np.cos(angle), -weight * np.sin(angle)], axis=1)
    return forward, inverse.reshape(NZ, NZ)


def plane_tables():
    c = np.arange(128)[:, None]
    b = np.arange(128)[None, :]
    out = []
    for d in range(4):
        angle = 2.0 * np.pi * (b * (4 * c + d) % 512) / 512
        cos, sin = np.cos(angle), np.sin(angle)
        out.append(np.block([[cos, sin], [-sin, cos]]))
    full = np.stack(out)
    return full, full.transpose(0, 2, 1)


def parts(value):
    high = value.astype(bf16)
    return high, (value - high.astype(f32)).astype(bf16)


def product(left, right, dims):
    dot = functools.partial(
        lax.dot_general, dimension_numbers=(dims, ((), ())), preferred_element_type=f32
    )
    return dot(left[0], right[0]) + (dot(left[0], right[1]) + dot(left[1], right[0]))


def spread(xr, xi):
    sr, si = xr[0] + xr[2], xi[0] + xi[2]
    tr, ti = xr[1] + xr[3], xi[1] + xi[3]
    pr, pi = xr[0] - xr[2], xi[0] - xi[2]
    qr, qi = xr[1] - xr[3], xi[1] - xi[3]
    return (
        (sr + tr, si + ti),
        (pr + qi, pi - qr),
        (sr - tr, si - ti),
        (pr - qi, pi + qr),
    )


def gather(vr, vi):
    sr, si = vr[0] + vr[2], vi[0] + vi[2]
    tr, ti = vr[1] + vr[3], vi[1] + vi[3]
    pr, pi = vr[0] - vr[2], vi[0] - vi[2]
    qr, qi = vr[1] - vr[3], vi[1] - vi[3]
    return (
        (sr + tr, si + ti),
        (pr - qi, pi + qr),
        (sr - tr, si - ti),
        (pr + qi, pi - qr),
    )


def wave(index):
    signed = jnp.where(index < 256, index, index - 512)
    return (2.0 * math.pi / 512) * signed.astype(f32)


def kernel(
    conc_hbm, tables_hbm,
    out, mass_ref,
    conc, tables, send_c, send_q, plane, back, got, retain, forcing,
    load_sem, local_sem, send_sem, recv_sem,
):
    slab = lax.axis_index("slab")
    pencil = lax.axis_index("pencil")
    me = slab * 64 + pencil

    barrier = pltpu.get_barrier_semaphore()

    def greet(step, carry):
        to = lax.rem(me + step, DEVICES)
        pl.semaphore_signal(
            barrier,
            inc=1,
            device_id=(lax.div(to, 64), lax.rem(to, 64)),
            device_id_type=MESH,
        )
        return carry

    loads = [
        pltpu.make_async_copy(src, dst, load_sem.at[i])
        for i, (src, dst) in enumerate(
            [
                (conc_hbm.at[:, 0:128], conc.at[0]),
                (conc_hbm.at[:, 128:256], conc.at[1]),
                (tables_hbm.at[0:2], tables.at[0:2]),
                (tables_hbm.at[2:20], tables.at[2:20]),
            ]
        )
    ]
    for load in loads:
        load.start()
    lax.fori_loop(1, DEVICES, greet, 0)
    for load in loads[:3]:
        load.wait()

    def table(first):
        return tables[first], tables[first + 1]

    def forward_table(d):
        return table(4 + 2 * d)

    def turned_table(d):
        return table(12 + 2 * d)

    def depth_forward(cubed, sends, h):
        def body(j, carry):
            value = jnp.concatenate(
                [
                    jnp.concatenate(
                        [
                            conc[i, pl.ds(h * HALF * COLS + 2 * j + e, HALF, stride=COLS), :]
                            for i in range(2)
                        ],
                        axis=1,
                    )
                    for e in range(2)
                ],
                axis=0,
            )
            if cubed:
                value = value * value * value
            result = product(table(0), parts(value), ((1,), (1,)))
            for i in range(2):
                for e in range(2):
                    sends[h, pl.ds(i * COLS + 2 * j + e, KEPT, stride=2 * COLS), :] = result[
                        i * KEPT : (i + 1) * KEPT, e * HALF : (e + 1) * HALF
                    ]
            return carry

        lax.fori_loop(0, COLS // 2, body, 0)

    def forward_block(sends, field, h, to_slab, to_pencil):
        return (
            sends.at[
                h, pl.ds(pl.multiple_of(to_slab * 1024 + to_pencil * 16, 16), 16), :
            ].reshape(2, 8, 128),
            plane.at[
                2 * field : 2 * field + 2,
                pl.ds(pl.multiple_of(pencil * COLS, COLS), COLS),
                pl.ds(pl.multiple_of(slab * ROWS + h * HALF, HALF), HALF),
            ],
        )

    def backward_block(h, to_slab, to_pencil):
        return (
            back.at[
                :,
                pl.ds(pl.multiple_of(to_pencil * COLS, COLS), COLS),
                pl.ds(pl.multiple_of(to_slab * ROWS + h * HALF, HALF), HALF),
            ],
            got.at[h, pl.ds(pl.multiple_of(me * 16, 16), 16), :].reshape(2, 8, 128),
        )

    def keep_own(block, stage):
        src, dst = block(slab, pencil)
        pltpu.make_async_copy(src, dst, local_sem.at[stage]).start()

    def exchange(block, stage, core):
        def send(to_slab, to_pencil):
            src, dst = block(to_slab, to_pencil)
            pltpu.make_async_remote_copy(
                src_ref=src,
                dst_ref=dst,
                send_sem=send_sem.at[stage],
                recv_sem=recv_sem.at[stage],
                device_id=(to_slab, to_pencil),
                device_id_type=MESH,
            ).start()

        chip = lax.div(pencil, 2)

        def pair(turn, carry):
            to_pencil = 2 * lax.rem(chip + 11 * turn, 32) + core
            send(slab, to_pencil)
            send(1 - slab, to_pencil)
            return carry

        lax.fori_loop(1, 32, pair, 0)
        send(1 - slab, 2 * chip + core)

        @pl.when(lax.rem(pencil, 2) != core)
        def _():
            send(slab, 2 * chip + core)

    def arrived(block, stage):
        src, dst = block(slab, pencil)
        pltpu.make_async_copy(src, dst, local_sem.at[stage]).wait()
        rows = pl.ds(0, 16 * (DEVICES - 1))
        everything = pltpu.make_async_remote_copy(
            src_ref=got.at[0, rows, :],
            dst_ref=got.at[0, rows, :],
            send_sem=send_sem.at[stage],
            recv_sem=recv_sem.at[stage],
            device_id=(slab, pencil),
            device_id_type=MESH,
        )
        everything.wait()

    def lane_halves(h):
        return [slice(i * ROWS + h * HALF, i * ROWS + (h + 1) * HALF) for i in range(2)]

    def both(index, rows, h):
        return jnp.concatenate([plane[index, rows, lanes] for lanes in lane_halves(h)], axis=1)

    def second_forward(field, h):
        quarters = [slice(a * 128, (a + 1) * 128) for a in range(4)]
        xr = [both(2 * field, rows, h) for rows in quarters]
        xi = [both(2 * field + 1, rows, h) for rows in quarters]
        for d, (ur, ui) in enumerate(spread(xr, xi)):
            result = product(
                forward_table(d), parts(jnp.concatenate([ur, ui], axis=0)), ((1,), (0,))
            )
            for i, lanes in enumerate(lane_halves(h)):
                half = slice(i * HALF, (i + 1) * HALF)
                plane[2 * field, quarters[d], lanes] = result[:128, half]
                plane[2 * field + 1, quarters[d], lanes] = result[128:, half]

    def first_forward(field, rows):
        xr = [plane[2 * field, rows, a * 128 : (a + 1) * 128] for a in range(4)]
        xi = [plane[2 * field + 1, rows, a * 128 : (a + 1) * 128] for a in range(4)]
        return [
            product(parts(jnp.concatenate([ur, ui], axis=1)), turned_table(d), ((1,), (0,)))
            for d, (ur, ui) in enumerate(spread(xr, xi))
        ]

    def row_block(i):
        return pl.ds(pl.multiple_of(i * 128, 128), 128)

    def first_forward_conc():
        def body(i, carry):
            rows = row_block(i)
            for d, result in enumerate(first_forward(0, rows)):
                plane[0, rows, d * 128 : (d + 1) * 128] = result[:, :128]
                plane[1, rows, d * 128 : (d + 1) * 128] = result[:, 128:]
            return carry

        lax.fori_loop(0, 4, body, 0)

    def multipliers():
        third = wave(me) * (512 // NZ)

        def body(i, carry):
            rows = row_block(i)
            row = lax.broadcasted_iota(jnp.int32, (128, 512), 0)
            lane = lax.broadcasted_iota(jnp.int32, (128, 512), 1)
            second = wave(row * 4 + i)
            first = wave(lane % 128 * 4 + lane // 128)
            square = first * first + second * second + third * third
            divisor = 1.0 + time_step * stiffness * square * square
            retain[rows, :] = (1.0 + time_step * square) / divisor
            forcing[rows, :] = (time_step * square) / divisor
            return carry

        lax.fori_loop(0, 4, body, 0)

    def combine_and_first_inverse():
        def body(i, carry):
            rows = row_block(i)
            vr, vi = [], []
            for d, cube in enumerate(first_forward(1, rows)):
                lanes = slice(d * 128, (d + 1) * 128)
                keep, force = retain[rows, lanes], forcing[rows, lanes]
                next_real = keep * plane[0, rows, lanes] - force * cube[:, :128]
                next_imag = keep * plane[1, rows, lanes] - force * cube[:, 128:]
                result = product(
                    parts(jnp.concatenate([next_real, next_imag], axis=1)),
                    forward_table(d),
                    ((1,), (0,)),
                )
                vr.append(result[:, :128])
                vi.append(result[:, 128:])
            for a, (xr, xi) in enumerate(gather(vr, vi)):
                plane[2, rows, a * 128 : (a + 1) * 128] = xr
                plane[3, rows, a * 128 : (a + 1) * 128] = xi
            return carry

        lax.fori_loop(0, 4, body, 0)

    def second_inverse(h, mass):
        quarters = [slice(a * 128, (a + 1) * 128) for a in range(4)]
        vr, vi = [], []
        for d in range(4):
            value = jnp.concatenate([both(2, quarters[d], h), both(3, quarters[d], h)], axis=0)
            result = product(turned_table(d), parts(value), ((1,), (0,)))
            vr.append(result[:128])
            vi.append(result[128:])
        for a, (xr, xi) in enumerate(gather(vr, vi)):
            xi = jnp.where(me == 0, mass, xi)
            for i, lanes in enumerate(lane_halves(h)):
                half = slice(i * HALF, (i + 1) * HALF)
                back[0, quarters[a], lanes] = xr[:, half]
                back[1, quarters[a], lanes] = xi[:, half]

    def depth_inverse(h):
        def body(j, carry):
            value = jnp.concatenate(
                [got[h, pl.ds(2 * j + e, NZ, stride=COLS), :] for e in range(2)], axis=1
            )
            result = product(parts(value), table(2), ((0,), (0,)))
            for e in range(2):
                for i in range(2):
                    out[i, pl.ds(h * HALF * COLS + 2 * j + e, HALF, stride=COLS), :] = result[
                        e * HALF : (e + 1) * HALF, i * 128 : (i + 1) * 128
                    ]
            return carry

        lax.fori_loop(0, COLS // 2, body, 0)

    def forward_stage(stage):
        sends = send_c if stage < 2 else send_q
        return functools.partial(forward_block, sends, stage // 2, stage % 2)

    for stage in range(4):
        depth_forward(stage >= 2, send_c if stage < 2 else send_q, stage % 2)
        if stage == 0:
            pl.semaphore_wait(barrier, DEVICES - 1)
        keep_own(forward_stage(stage), stage)
        exchange(forward_stage(stage), stage, FIRST)
    for stage in range(4):
        exchange(forward_stage(stage), stage, 1 - FIRST)
    multipliers()
    loads[3].wait()
    for h in range(2):
        arrived(forward_stage(h), h)
        second_forward(0, h)
    first_forward_conc()
    mass = jnp.broadcast_to(plane[0, 0:1, 0:1], (128, 256)) * (1.0 / TOTAL)
    for h in range(2):
        arrived(forward_stage(2 + h), 2 + h)
        second_forward(1, h)
    combine_and_first_inverse()
    for h in range(2):
        block = functools.partial(backward_block, h)
        second_inverse(h, mass)
        keep_own(block, 4 + h)
        for core in range(2):
            exchange(block, 4 + h, core)
    for h in range(2):
        arrived(functools.partial(backward_block, h), 4 + h)
        depth_inverse(h)
    mass_ref[...] = got[0, 8:16, :]


def deliver(parts_ref, mass_in, out_hbm, mass_ref, sem):
    copies = [
        pltpu.make_async_copy(
            parts_ref.at[i], out_hbm.at[:, i * 128 : (i + 1) * 128], sem.at[i]
        )
        for i in range(2)
    ]
    for copy in copies:
        copy.start()
    mass_ref[...] = mass_in[0:1, 0:1]
    for copy in copies:
        copy.wait()


def local(concentration):
    tables = all_tables()
    anywhere = pl.BlockSpec(memory_space=pl.ANY)
    vmem = pl.BlockSpec(memory_space=pltpu.VMEM)
    halves, mass = pl.pallas_call(
        kernel,
        out_shape=(
            jax.ShapeDtypeStruct((2, ROWS * COLS, 128), f32),
            jax.ShapeDtypeStruct((8, 128), f32),
        ),
        in_specs=[anywhere] * 2,
        out_specs=(vmem, vmem),
        scratch_shapes=[
            pltpu.VMEM((2, ROWS * COLS, 128), f32),
            pltpu.VMEM(tables.shape, bf16),
            pltpu.VMEM((2, KEPT * 16, HALF), f32),
            pltpu.VMEM((2, KEPT * 16, HALF), f32),
            pltpu.VMEM((4, NY, NX), f32),
            pltpu.VMEM((2, NY, NX), f32),
            pltpu.VMEM((2, KEPT * 16, HALF), f32),
            pltpu.VMEM((NY, NX), f32),
            pltpu.VMEM((NY, NX), f32),
            pltpu.SemaphoreType.DMA((4,)),
            pltpu.SemaphoreType.DMA((6,)),
            pltpu.SemaphoreType.DMA((6,)),
            pltpu.SemaphoreType.DMA((6,)),
        ],
        compiler_params=pltpu.CompilerParams(
            collective_id=0, has_side_effects=True, vmem_limit_bytes=50 * 2**20
        ),
        name="cahn_hilliard_step",
    )(
        concentration.reshape(ROWS * COLS, NZ),
        jnp.asarray(tables),
    )
    updated, mass = pl.pallas_call(
        deliver,
        out_shape=(
            jax.ShapeDtypeStruct((ROWS * COLS, NZ), f32),
            jax.ShapeDtypeStruct((1, 1), f32),
        ),
        in_specs=[vmem, vmem],
        out_specs=(anywhere, vmem),
        scratch_shapes=[pltpu.SemaphoreType.DMA((2,))],
        compiler_params=pltpu.CompilerParams(vmem_limit_bytes=8 * 2**20),
        name="deliver",
    )(halves, mass)
    return updated.reshape(ROWS, COLS, NZ), mass.reshape(())


def solution(mesh):
    return jax.shard_map(
        local,
        mesh=mesh,
        in_specs=(P("slab", "pencil", None),),
        out_specs=(P("slab", "pencil", None), P()),
        check_vma=False,
    )
```

```python
import functools
import math

import jax
import jax.numpy as jnp
import numpy as np
from jax import lax
from jax.experimental import pallas as pl
from jax.experimental.pallas import tpu as pltpu
from jax.sharding import PartitionSpec as P

NX = 512
NY = 512
NZ = 256
KEPT = NZ // 2
DEVICES = 128
ROWS = 256
COLS = 8
HALF = ROWS // 2
TOTAL = NX * NY * NZ
FIRST = 1

time_step = 1.0
stiffness = 1.0

MESH = pl.DeviceIdType.MESH
f32 = jnp.float32
bf16 = jnp.bfloat16


def all_tables():
    full = np.concatenate([depth_tables(), *plane_tables()])
    high = full.astype(np.float32).astype(bf16)
    low = (full - high.astype(np.float64)).astype(np.float32).astype(bf16)
    return np.stack([high, low], axis=1).reshape(20, 256, 256)


def depth_tables():
    k = np.arange(KEPT)[:, None]
    n = np.arange(NZ)[None, :]
    angle = 2.0 * np.pi * (k * n % NZ) / NZ
    forward = np.concatenate([np.cos(angle), -np.sin(angle)], axis=0)
    weight = np.where(k == 0, 1.0, 2.0) / TOTAL
    inverse = np.stack([weight * np.cos(angle), -weight * np.sin(angle)], axis=1)
    return forward, inverse.reshape(NZ, NZ)


def plane_tables():
    c = np.arange(128)[:, None]
    b = np.arange(128)[None, :]
    out = []
    for d in range(4):
        angle = 2.0 * np.pi * (b * (4 * c + d) % 512) / 512
        cos, sin = np.cos(angle), np.sin(angle)
        out.append(np.block([[cos, sin], [-sin, cos]]))
    full = np.stack(out)
    return full, full.transpose(0, 2, 1)


def parts(value):
    high = value.astype(bf16)
    return high, (value - high.astype(f32)).astype(bf16)


def product(left, right, dims):
    dot = functools.partial(
        lax.dot_general, dimension_numbers=(dims, ((), ())), preferred_element_type=f32
    )
    return dot(left[0], right[0]) + (dot(left[0], right[1]) + dot(left[1], right[0]))


def spread(xr, xi):
    sr, si = xr[0] + xr[2], xi[0] + xi[2]
    tr, ti = xr[1] + xr[3], xi[1] + xi[3]
    pr, pi = xr[0] - xr[2], xi[0] - xi[2]
    qr, qi = xr[1] - xr[3], xi[1] - xi[3]
    return (
        (sr + tr, si + ti),
        (pr + qi, pi - qr),
        (sr - tr, si - ti),
        (pr - qi, pi + qr),
    )


def gather(vr, vi):
    sr, si = vr[0] + vr[2], vi[0] + vi[2]
    tr, ti = vr[1] + vr[3], vi[1] + vi[3]
    pr, pi = vr[0] - vr[2], vi[0] - vi[2]
    qr, qi = vr[1] - vr[3], vi[1] - vi[3]
    return (
        (sr + tr, si + ti),
        (pr - qi, pi + qr),
        (sr - tr, si - ti),
        (pr + qi, pi - qr),
    )


def wave(index):
    signed = jnp.where(index < 256, index, index - 512)
    return (2.0 * math.pi / 512) * signed.astype(f32)


def kernel(
    conc_hbm, tables_hbm,
    out, mass_ref,
    conc, tables, send_c, send_q, plane, back, got, retain, forcing,
    load_sem, local_sem, send_sem, recv_sem,
):
    slab = lax.axis_index("slab")
    pencil = lax.axis_index("pencil")
    me = slab * 64 + pencil

    barrier = pltpu.get_barrier_semaphore()

    def greet(step, carry):
        to = lax.rem(me + step, DEVICES)
        pl.semaphore_signal(
            barrier,
            inc=1,
            device_id=(lax.div(to, 64), lax.rem(to, 64)),
            device_id_type=MESH,
        )
        return carry

    loads = [
        pltpu.make_async_copy(src, dst, load_sem.at[i])
        for i, (src, dst) in enumerate(
            [
                (conc_hbm.at[:, 0:128], conc.at[0]),
                (conc_hbm.at[:, 128:256], conc.at[1]),
                (tables_hbm.at[0:2], tables.at[0:2]),
                (tables_hbm.at[2:20], tables.at[2:20]),
            ]
        )
    ]
    for load in loads:
        load.start()
    lax.fori_loop(1, DEVICES, greet, 0)
    for load in loads[:3]:
        load.wait()

    def table(first):
        return tables[first], tables[first + 1]

    def forward_table(d):
        return table(4 + 2 * d)

    def turned_table(d):
        return table(12 + 2 * d)

    def depth_forward(cubed, sends, h):
        def body(j, carry):
            value = jnp.concatenate(
                [
                    jnp.concatenate(
                        [
                            conc[i, pl.ds(h * HALF * COLS + 2 * j + e, HALF, stride=COLS), :]
                            for i in range(2)
                        ],
                        axis=1,
                    )
                    for e in range(2)
                ],
                axis=0,
            )
            if cubed:
                value = value * value * value
            result = product(table(0), parts(value), ((1,), (1,)))
            for i in range(2):
                for e in range(2):
                    sends[h, pl.ds(i * COLS + 2 * j + e, KEPT, stride=2 * COLS), :] = result[
                        i * KEPT : (i + 1) * KEPT, e * HALF : (e + 1) * HALF
                    ]
            return carry

        lax.fori_loop(0, COLS // 2, body, 0)

    def forward_block(sends, field, h, to_slab, to_pencil):
        return (
            sends.at[
                h, pl.ds(pl.multiple_of(to_slab * 1024 + to_pencil * 16, 16), 16), :
            ].reshape(2, 8, 128),
            plane.at[
                2 * field : 2 * field + 2,
                pl.ds(pl.multiple_of(pencil * COLS, COLS), COLS),
                pl.ds(pl.multiple_of(slab * ROWS + h * HALF, HALF), HALF),
            ],
        )

    def backward_block(h, to_slab, to_pencil):
        return (
            back.at[
                :,
                pl.ds(pl.multiple_of(to_pencil * COLS, COLS), COLS),
                pl.ds(pl.multiple_of(to_slab * ROWS + h * HALF, HALF), HALF),
            ],
            got.at[h, pl.ds(pl.multiple_of(me * 16, 16), 16), :].reshape(2, 8, 128),
        )

    def keep_own(block, stage):
        src, dst = block(slab, pencil)
        pltpu.make_async_copy(src, dst, local_sem.at[stage]).start()

    def exchange(block, stage, core):
        def send(to_slab, to_pencil):
            src, dst = block(to_slab, to_pencil)
            pltpu.make_async_remote_copy(
                src_ref=src,
                dst_ref=dst,
                send_sem=send_sem.at[stage],
                recv_sem=recv_sem.at[stage],
                device_id=(to_slab, to_pencil),
                device_id_type=MESH,
            ).start()

        chip = lax.div(pencil, 2)

        def pair(turn, carry):
            to_pencil = 2 * lax.rem(chip + 11 * turn, 32) + core
            send(slab, to_pencil)
            send(1 - slab, to_pencil)
            return carry

        lax.fori_loop(1, 32, pair, 0)
        send(1 - slab, 2 * chip + core)

        @pl.when(lax.rem(pencil, 2) != core)
        def _():
            send(slab, 2 * chip + core)

    def everything(stage):
        rows = pl.ds(0, 16 * (DEVICES - 1))
        return pltpu.make_async_remote_copy(
            src_ref=got.at[0, rows, :],
            dst_ref=got.at[0, rows, :],
            send_sem=send_sem.at[stage],
            recv_sem=recv_sem.at[stage],
            device_id=(slab, pencil),
            device_id_type=MESH,
        )

    def arrived(block, stage):
        src, dst = block(slab, pencil)
        pltpu.make_async_copy(src, dst, local_sem.at[stage]).wait()
        everything(stage).wait_recv()

    def lane_halves(h):
        return [slice(i * ROWS + h * HALF, i * ROWS + (h + 1) * HALF) for i in range(2)]

    def both(index, rows, h):
        return jnp.concatenate([plane[index, rows, lanes] for lanes in lane_halves(h)], axis=1)

    def second_forward(field, h):
        quarters = [slice(a * 128, (a + 1) * 128) for a in range(4)]
        xr = [both(2 * field, rows, h) for rows in quarters]
        xi = [both(2 * field + 1, rows, h) for rows in quarters]
        for d, (ur, ui) in enumerate(spread(xr, xi)):
            result = product(
                forward_table(d), parts(jnp.concatenate([ur, ui], axis=0)), ((1,), (0,))
            )
            for i, lanes in enumerate(lane_halves(h)):
                half = slice(i * HALF, (i + 1) * HALF)
                plane[2 * field, quarters[d], lanes] = result[:128, half]
                plane[2 * field + 1, quarters[d], lanes] = result[128:, half]

    def first_forward(field, rows):
        xr = [plane[2 * field, rows, a * 128 : (a + 1) * 128] for a in range(4)]
        xi = [plane[2 * field + 1, rows, a * 128 : (a + 1) * 128] for a in range(4)]
        return [
            product(parts(jnp.concatenate([ur, ui], axis=1)), turned_table(d), ((1,), (0,)))
            for d, (ur, ui) in enumerate(spread(xr, xi))
        ]

    def row_block(i):
        return pl.ds(pl.multiple_of(i * 128, 128), 128)

    def first_forward_conc():
        def body(i, carry):
            rows = row_block(i)
            for d, result in enumerate(first_forward(0, rows)):
                plane[0, rows, d * 128 : (d + 1) * 128] = result[:, :128]
                plane[1, rows, d * 128 : (d + 1) * 128] = result[:, 128:]
            return carry

        lax.fori_loop(0, 4, body, 0)

    def multipliers():
        third = wave(me) * (512 // NZ)

        def body(i, carry):
            rows = row_block(i)
            row = lax.broadcasted_iota(jnp.int32, (128, 512), 0)
            lane = lax.broadcasted_iota(jnp.int32, (128, 512), 1)
            second = wave(row * 4 + i)
            first = wave(lane % 128 * 4 + lane // 128)
            square = first * first + second * second + third * third
            divisor = 1.0 + time_step * stiffness * square * square
            retain[rows, :] = (1.0 + time_step * square) / divisor
            forcing[rows, :] = (time_step * square) / divisor
            return carry

        lax.fori_loop(0, 4, body, 0)

    def combine_and_first_inverse():
        def body(i, carry):
            rows = row_block(i)
            vr, vi = [], []
            for d, cube in enumerate(first_forward(1, rows)):
                lanes = slice(d * 128, (d + 1) * 128)
                keep, force = retain[rows, lanes], forcing[rows, lanes]
                next_real = keep * plane[0, rows, lanes] - force * cube[:, :128]
                next_imag = keep * plane[1, rows, lanes] - force * cube[:, 128:]
                result = product(
                    parts(jnp.concatenate([next_real, next_imag], axis=1)),
                    forward_table(d),
                    ((1,), (0,)),
                )
                vr.append(result[:, :128])
                vi.append(result[:, 128:])
            for a, (xr, xi) in enumerate(gather(vr, vi)):
                plane[2, rows, a * 128 : (a + 1) * 128] = xr
                plane[3, rows, a * 128 : (a + 1) * 128] = xi
            return carry

        lax.fori_loop(0, 4, body, 0)

    def second_inverse(h, mass):
        quarters = [slice(a * 128, (a + 1) * 128) for a in range(4)]
        vr, vi = [], []
        for d in range(4):
            value = jnp.concatenate([both(2, quarters[d], h), both(3, quarters[d], h)], axis=0)
            result = product(turned_table(d), parts(value), ((1,), (0,)))
            vr.append(result[:128])
            vi.append(result[128:])
        for a, (xr, xi) in enumerate(gather(vr, vi)):
            xi = jnp.where(me == 0, mass, xi)
            for i, lanes in enumerate(lane_halves(h)):
                half = slice(i * HALF, (i + 1) * HALF)
                back[0, quarters[a], lanes] = xr[:, half]
                back[1, quarters[a], lanes] = xi[:, half]

    def depth_inverse(h):
        def body(j, carry):
            value = jnp.concatenate(
                [got[h, pl.ds(2 * j + e, NZ, stride=COLS), :] for e in range(2)], axis=1
            )
            result = product(parts(value), table(2), ((0,), (0,)))
            for e in range(2):
                for i in range(2):
                    out[i, pl.ds(h * HALF * COLS + 2 * j + e, HALF, stride=COLS), :] = result[
                        e * HALF : (e + 1) * HALF, i * 128 : (i + 1) * 128
                    ]
            return carry

        lax.fori_loop(0, COLS // 2, body, 0, unroll=True)

    def forward_stage(stage):
        sends = send_c if stage < 2 else send_q
        return functools.partial(forward_block, sends, stage // 2, stage % 2)

    for stage in range(4):
        depth_forward(stage >= 2, send_c if stage < 2 else send_q, stage % 2)
        if stage == 0:
            pl.semaphore_wait(barrier, DEVICES - 1)
        keep_own(forward_stage(stage), stage)
        exchange(forward_stage(stage), stage, FIRST)
    for stage in range(4):
        exchange(forward_stage(stage), stage, 1 - FIRST)
    multipliers()
    loads[3].wait()
    for h in range(2):
        arrived(forward_stage(h), h)
        second_forward(0, h)
    first_forward_conc()
    mass = jnp.broadcast_to(plane[0, 0:1, 0:1], (128, 256)) * (1.0 / TOTAL)
    for h in range(2):
        arrived(forward_stage(2 + h), 2 + h)
        second_forward(1, h)
    combine_and_first_inverse()
    for h in range(2):
        block = functools.partial(backward_block, h)
        second_inverse(h, mass)
        keep_own(block, 4 + h)
        for core in range(2):
            exchange(block, 4 + h, core)
    for h in range(2):
        arrived(functools.partial(backward_block, h), 4 + h)
        depth_inverse(h)
    mass_ref[...] = got[0, 8:16, :]
    for stage in range(6):
        everything(stage).wait_send()


def deliver(parts_ref, mass_in, out_hbm, mass_ref, sem):
    copies = [
        pltpu.make_async_copy(
            parts_ref.at[i], out_hbm.at[:, i * 128 : (i + 1) * 128], sem.at[i]
        )
        for i in range(2)
    ]
    for copy in copies:
        copy.start()
    mass_ref[...] = mass_in[0:1, 0:1]
    for copy in copies:
        copy.wait()


def local(concentration):
    tables = all_tables()
    anywhere = pl.BlockSpec(memory_space=pl.ANY)
    vmem = pl.BlockSpec(memory_space=pltpu.VMEM)
    halves, mass = pl.pallas_call(
        kernel,
        out_shape=(
            jax.ShapeDtypeStruct((2, ROWS * COLS, 128), f32),
            jax.ShapeDtypeStruct((8, 128), f32),
        ),
        in_specs=[anywhere] * 2,
        out_specs=(vmem, vmem),
        scratch_shapes=[
            pltpu.VMEM((2, ROWS * COLS, 128), f32),
            pltpu.VMEM(tables.shape, bf16),
            pltpu.VMEM((2, KEPT * 16, HALF), f32),
            pltpu.VMEM((2, KEPT * 16, HALF), f32),
            pltpu.VMEM((4, NY, NX), f32),
            pltpu.VMEM((2, NY, NX), f32),
            pltpu.VMEM((2, KEPT * 16, HALF), f32),
            pltpu.VMEM((NY, NX), f32),
            pltpu.VMEM((NY, NX), f32),
            pltpu.SemaphoreType.DMA((4,)),
            pltpu.SemaphoreType.DMA((6,)),
            pltpu.SemaphoreType.DMA((6,)),
            pltpu.SemaphoreType.DMA((6,)),
        ],
        compiler_params=pltpu.CompilerParams(
            collective_id=0, has_side_effects=True, vmem_limit_bytes=50 * 2**20
        ),
        name="cahn_hilliard_step",
    )(
        concentration.reshape(ROWS * COLS, NZ),
        jnp.asarray(tables),
    )
    updated, mass = pl.pallas_call(
        deliver,
        out_shape=(
            jax.ShapeDtypeStruct((ROWS * COLS, NZ), f32),
            jax.ShapeDtypeStruct((1, 1), f32),
        ),
        in_specs=[vmem, vmem],
        out_specs=(anywhere, vmem),
        scratch_shapes=[pltpu.SemaphoreType.DMA((2,))],
        compiler_params=pltpu.CompilerParams(vmem_limit_bytes=8 * 2**20),
        name="deliver",
    )(halves, mass)
    return updated.reshape(ROWS, COLS, NZ), mass.reshape(())


def solution(mesh):
    return jax.shard_map(
        local,
        mesh=mesh,
        in_specs=(P("slab", "pencil", None),),
        out_specs=(P("slab", "pencil", None), P()),
        check_vma=False,
    )
```

```python
import functools
import math

import jax
import jax.numpy as jnp
import numpy as np
from jax import lax
from jax.experimental import pallas as pl
from jax.experimental.pallas import tpu as pltpu
from jax.sharding import PartitionSpec as P

NX = 512
NY = 512
NZ = 256
KEPT = NZ // 2
DEVICES = 128
ROWS = 256
COLS = 8
HALF = ROWS // 2
TOTAL = NX * NY * NZ
NEAR_LAST = [22, 23, 13, 14, 15, 26, 6, 17, 18, 29, 19, 30, 20, 31, 10, 21, 11, 12, 2, 25, 5, 16, 27, 28, 7, 9, 1, 24, 3, 4, 8]
FIRST = 1

time_step = 1.0
stiffness = 1.0

MESH = pl.DeviceIdType.MESH
f32 = jnp.float32
bf16 = jnp.bfloat16


def all_tables():
    full = np.concatenate([depth_tables(), *plane_tables()])
    high = full.astype(np.float32).astype(bf16)
    low = (full - high.astype(np.float64)).astype(np.float32).astype(bf16)
    return np.stack([high, low], axis=1).reshape(20, 256, 256)


def depth_tables():
    k = np.arange(KEPT)[:, None]
    n = np.arange(NZ)[None, :]
    angle = 2.0 * np.pi * (k * n % NZ) / NZ
    forward = np.concatenate([np.cos(angle), -np.sin(angle)], axis=0)
    weight = np.where(k == 0, 1.0, 2.0) / TOTAL
    inverse = np.stack([weight * np.cos(angle), -weight * np.sin(angle)], axis=1)
    return forward, inverse.reshape(NZ, NZ)


def plane_tables():
    c = np.arange(128)[:, None]
    b = np.arange(128)[None, :]
    out = []
    for d in range(4):
        angle = 2.0 * np.pi * (b * (4 * c + d) % 512) / 512
        cos, sin = np.cos(angle), np.sin(angle)
        out.append(np.block([[cos, sin], [-sin, cos]]))
    full = np.stack(out)
    return full, full.transpose(0, 2, 1)


def parts(value):
    high = value.astype(bf16)
    return high, (value - high.astype(f32)).astype(bf16)


def product(left, right, dims):
    dot = functools.partial(
        lax.dot_general, dimension_numbers=(dims, ((), ())), preferred_element_type=f32
    )
    return dot(left[0], right[0]) + (dot(left[0], right[1]) + dot(left[1], right[0]))


def spread(xr, xi):
    sr, si = xr[0] + xr[2], xi[0] + xi[2]
    tr, ti = xr[1] + xr[3], xi[1] + xi[3]
    pr, pi = xr[0] - xr[2], xi[0] - xi[2]
    qr, qi = xr[1] - xr[3], xi[1] - xi[3]
    return (
        (sr + tr, si + ti),
        (pr + qi, pi - qr),
        (sr - tr, si - ti),
        (pr - qi, pi + qr),
    )


def gather(vr, vi):
    sr, si = vr[0] + vr[2], vi[0] + vi[2]
    tr, ti = vr[1] + vr[3], vi[1] + vi[3]
    pr, pi = vr[0] - vr[2], vi[0] - vi[2]
    qr, qi = vr[1] - vr[3], vi[1] - vi[3]
    return (
        (sr + tr, si + ti),
        (pr - qi, pi + qr),
        (sr - tr, si - ti),
        (pr + qi, pi - qr),
    )


def wave(index):
    signed = jnp.where(index < 256, index, index - 512)
    return (2.0 * math.pi / 512) * signed.astype(f32)


def kernel(
    conc_hbm, tables_hbm,
    out, mass_ref,
    conc, tables, send_c, send_q, plane, back, got, retain, forcing,
    load_sem, local_sem, send_sem, recv_sem,
):
    slab = lax.axis_index("slab")
    pencil = lax.axis_index("pencil")
    me = slab * 64 + pencil

    barrier = pltpu.get_barrier_semaphore()

    def greet(step, carry):
        to = lax.rem(me + step, DEVICES)
        pl.semaphore_signal(
            barrier,
            inc=1,
            device_id=(lax.div(to, 64), lax.rem(to, 64)),
            device_id_type=MESH,
        )
        return carry

    loads = [
        pltpu.make_async_copy(src, dst, load_sem.at[i])
        for i, (src, dst) in enumerate(
            [
                (conc_hbm.at[:, 0:128], conc.at[0]),
                (conc_hbm.at[:, 128:256], conc.at[1]),
                (tables_hbm.at[0:2], tables.at[0:2]),
                (tables_hbm.at[2:20], tables.at[2:20]),
            ]
        )
    ]
    for load in loads:
        load.start()
    lax.fori_loop(1, DEVICES, greet, 0)
    for load in loads[:3]:
        load.wait()

    def table(first):
        return tables[first], tables[first + 1]

    def forward_table(d):
        return table(4 + 2 * d)

    def turned_table(d):
        return table(12 + 2 * d)

    def depth_forward(cubed, sends, h):
        def body(j, carry):
            value = jnp.concatenate(
                [
                    jnp.concatenate(
                        [
                            conc[i, pl.ds(h * HALF * COLS + 2 * j + e, HALF, stride=COLS), :]
                            for i in range(2)
                        ],
                        axis=1,
                    )
                    for e in range(2)
                ],
                axis=0,
            )
            if cubed:
                value = value * value * value
            result = product(table(0), parts(value), ((1,), (1,)))
            for i in range(2):
                for e in range(2):
                    sends[h, pl.ds(i * COLS + 2 * j + e, KEPT, stride=2 * COLS), :] = result[
                        i * KEPT : (i + 1) * KEPT, e * HALF : (e + 1) * HALF
                    ]
            return carry

        lax.fori_loop(0, COLS // 2, body, 0, unroll=True)

    def forward_block(sends, field, h, to_slab, to_pencil):
        return (
            sends.at[
                h, pl.ds(pl.multiple_of(to_slab * 1024 + to_pencil * 16, 16), 16), :
            ].reshape(2, 8, 128),
            plane.at[
                2 * field : 2 * field + 2,
                pl.ds(pl.multiple_of(pencil * COLS, COLS), COLS),
                pl.ds(pl.multiple_of(slab * ROWS + h * HALF, HALF), HALF),
            ],
        )

    def backward_block(h, to_slab, to_pencil):
        return (
            back.at[
                :,
                pl.ds(pl.multiple_of(to_pencil * COLS, COLS), COLS),
                pl.ds(pl.multiple_of(to_slab * ROWS + h * HALF, HALF), HALF),
            ],
            got.at[h, pl.ds(pl.multiple_of(me * 16, 16), 16), :].reshape(2, 8, 128),
        )

    def keep_own(block, stage):
        src, dst = block(slab, pencil)
        pltpu.make_async_copy(src, dst, local_sem.at[stage]).start()

    def exchange(block, stage, core):
        def send(to_slab, to_pencil):
            src, dst = block(to_slab, to_pencil)
            pltpu.make_async_remote_copy(
                src_ref=src,
                dst_ref=dst,
                send_sem=send_sem.at[stage],
                recv_sem=recv_sem.at[stage],
                device_id=(to_slab, to_pencil),
                device_id_type=MESH,
            ).start()

        chip = lax.div(pencil, 2)

        def pair(turn, carry):
            to_pencil = 2 * lax.rem(chip + 11 * turn, 32) + core
            send(slab, to_pencil)
            send(1 - slab, to_pencil)
            return carry

        if stage < 4:
            lax.fori_loop(1, 32, pair, 0)
        else:
            for turn in NEAR_LAST:
                to_pencil = 2 * lax.rem(chip + turn, 32) + core
                send(1 - slab, to_pencil)
                send(slab, to_pencil)
        send(1 - slab, 2 * chip + core)

        @pl.when(lax.rem(pencil, 2) != core)
        def _():
            send(slab, 2 * chip + core)

    def everything(stage):
        rows = pl.ds(0, 16 * (DEVICES - 1))
        return pltpu.make_async_remote_copy(
            src_ref=got.at[0, rows, :],
            dst_ref=got.at[0, rows, :],
            send_sem=send_sem.at[stage],
            recv_sem=recv_sem.at[stage],
            device_id=(slab, pencil),
            device_id_type=MESH,
        )

    def arrived(block, stage):
        src, dst = block(slab, pencil)
        pltpu.make_async_copy(src, dst, local_sem.at[stage]).wait()
        everything(stage).wait_recv()

    def lane_halves(h):
        return [slice(i * ROWS + h * HALF, i * ROWS + (h + 1) * HALF) for i in range(2)]

    def both(index, rows, h):
        return jnp.concatenate([plane[index, rows, lanes] for lanes in lane_halves(h)], axis=1)

    def second_forward(field, h):
        quarters = [slice(a * 128, (a + 1) * 128) for a in range(4)]
        xr = [both(2 * field, rows, h) for rows in quarters]
        xi = [both(2 * field + 1, rows, h) for rows in quarters]
        for d, (ur, ui) in enumerate(spread(xr, xi)):
            result = product(
                forward_table(d), parts(jnp.concatenate([ur, ui], axis=0)), ((1,), (0,))
            )
            for i, lanes in enumerate(lane_halves(h)):
                half = slice(i * HALF, (i + 1) * HALF)
                plane[2 * field, quarters[d], lanes] = result[:128, half]
                plane[2 * field + 1, quarters[d], lanes] = result[128:, half]

    def first_forward(field, rows):
        xr = [plane[2 * field, rows, a * 128 : (a + 1) * 128] for a in range(4)]
        xi = [plane[2 * field + 1, rows, a * 128 : (a + 1) * 128] for a in range(4)]
        return [
            product(parts(jnp.concatenate([ur, ui], axis=1)), turned_table(d), ((1,), (0,)))
            for d, (ur, ui) in enumerate(spread(xr, xi))
        ]

    def row_block(i):
        return pl.ds(pl.multiple_of(i * 128, 128), 128)

    def first_forward_conc():
        def body(i, carry):
            rows = row_block(i)
            for d, result in enumerate(first_forward(0, rows)):
                plane[0, rows, d * 128 : (d + 1) * 128] = result[:, :128]
                plane[1, rows, d * 128 : (d + 1) * 128] = result[:, 128:]
            return carry

        lax.fori_loop(0, 4, body, 0)

    def multipliers():
        third = wave(me) * (512 // NZ)

        def body(i, carry):
            rows = row_block(i)
            row = lax.broadcasted_iota(jnp.int32, (128, 512), 0)
            lane = lax.broadcasted_iota(jnp.int32, (128, 512), 1)
            second = wave(row * 4 + i)
            first = wave(lane % 128 * 4 + lane // 128)
            square = first * first + second * second + third * third
            divisor = 1.0 + time_step * stiffness * square * square
            retain[rows, :] = (1.0 + time_step * square) / divisor
            forcing[rows, :] = (time_step * square) / divisor
            return carry

        lax.fori_loop(0, 4, body, 0)

    def combine_and_first_inverse():
        def body(i, carry):
            rows = row_block(i)
            vr, vi = [], []
            for d, cube in enumerate(first_forward(1, rows)):
                lanes = slice(d * 128, (d + 1) * 128)
                keep, force = retain[rows, lanes], forcing[rows, lanes]
                next_real = keep * plane[0, rows, lanes] - force * cube[:, :128]
                next_imag = keep * plane[1, rows, lanes] - force * cube[:, 128:]
                result = product(
                    parts(jnp.concatenate([next_real, next_imag], axis=1)),
                    forward_table(d),
                    ((1,), (0,)),
                )
                vr.append(result[:, :128])
                vi.append(result[:, 128:])
            for a, (xr, xi) in enumerate(gather(vr, vi)):
                plane[2, rows, a * 128 : (a + 1) * 128] = xr
                plane[3, rows, a * 128 : (a + 1) * 128] = xi
            return carry

        lax.fori_loop(0, 4, body, 0)

    def second_inverse(h, mass):
        quarters = [slice(a * 128, (a + 1) * 128) for a in range(4)]
        vr, vi = [], []
        for d in range(4):
            value = jnp.concatenate([both(2, quarters[d], h), both(3, quarters[d], h)], axis=0)
            result = product(turned_table(d), parts(value), ((1,), (0,)))
            vr.append(result[:128])
            vi.append(result[128:])
        for a, (xr, xi) in enumerate(gather(vr, vi)):
            xi = jnp.where(me == 0, mass, xi)
            for i, lanes in enumerate(lane_halves(h)):
                half = slice(i * HALF, (i + 1) * HALF)
                back[0, quarters[a], lanes] = xr[:, half]
                back[1, quarters[a], lanes] = xi[:, half]

    def depth_inverse(h):
        def body(j, carry):
            value = jnp.concatenate(
                [got[h, pl.ds(2 * j + e, NZ, stride=COLS), :] for e in range(2)], axis=1
            )
            result = product(parts(value), table(2), ((0,), (0,)))
            for e in range(2):
                for i in range(2):
                    out[i, pl.ds(h * HALF * COLS + 2 * j + e, HALF, stride=COLS), :] = result[
                        e * HALF : (e + 1) * HALF, i * 128 : (i + 1) * 128
                    ]
            return carry

        lax.fori_loop(0, COLS // 2, body, 0, unroll=True)

    def forward_stage(stage):
        sends = send_c if stage < 2 else send_q
        return functools.partial(forward_block, sends, stage // 2, stage % 2)

    for stage in range(4):
        depth_forward(stage >= 2, send_c if stage < 2 else send_q, stage % 2)
        if stage == 0:
            pl.semaphore_wait(barrier, DEVICES - 1)
        keep_own(forward_stage(stage), stage)
        exchange(forward_stage(stage), stage, FIRST)
    for stage in range(4):
        exchange(forward_stage(stage), stage, 1 - FIRST)
    multipliers()
    loads[3].wait()
    for h in range(2):
        arrived(forward_stage(h), h)
        second_forward(0, h)
    first_forward_conc()
    mass = jnp.broadcast_to(plane[0, 0:1, 0:1], (128, 256)) * (1.0 / TOTAL)
    for h in range(2):
        arrived(forward_stage(2 + h), 2 + h)
        second_forward(1, h)
    combine_and_first_inverse()
    for h in range(2):
        block = functools.partial(backward_block, h)
        second_inverse(h, mass)
        keep_own(block, 4 + h)
        exchange(block, 4 + h, FIRST)
    for h in range(2):
        exchange(functools.partial(backward_block, h), 4 + h, 1 - FIRST)
    for h in range(2):
        arrived(functools.partial(backward_block, h), 4 + h)
        depth_inverse(h)
    mass_ref[...] = got[0, 8:16, :]
    for stage in range(6):
        everything(stage).wait_send()


def deliver(parts_ref, mass_in, out_hbm, mass_ref, sem):
    copies = [
        pltpu.make_async_copy(
            parts_ref.at[i, r * 512 : (r + 1) * 512, :],
            out_hbm.at[r * 512 : (r + 1) * 512, i * 128 : (i + 1) * 128],
            sem.at[i, r],
        )
        for r in range(4)
        for i in range(2)
    ]
    for copy in copies:
        copy.start()
    mass_ref[...] = mass_in[0:1, 0:1]
    for copy in copies:
        copy.wait()


def local(concentration):
    tables = all_tables()
    anywhere = pl.BlockSpec(memory_space=pl.ANY)
    vmem = pl.BlockSpec(memory_space=pltpu.VMEM)
    halves, mass = pl.pallas_call(
        kernel,
        out_shape=(
            jax.ShapeDtypeStruct((2, ROWS * COLS, 128), f32),
            jax.ShapeDtypeStruct((8, 128), f32),
        ),
        in_specs=[anywhere] * 2,
        out_specs=(vmem, vmem),
        scratch_shapes=[
            pltpu.VMEM((2, ROWS * COLS, 128), f32),
            pltpu.VMEM(tables.shape, bf16),
            pltpu.VMEM((2, KEPT * 16, HALF), f32),
            pltpu.VMEM((2, KEPT * 16, HALF), f32),
            pltpu.VMEM((4, NY, NX), f32),
            pltpu.VMEM((2, NY, NX), f32),
            pltpu.VMEM((2, KEPT * 16, HALF), f32),
            pltpu.VMEM((NY, NX), f32),
            pltpu.VMEM((NY, NX), f32),
            pltpu.SemaphoreType.DMA((4,)),
            pltpu.SemaphoreType.DMA((6,)),
            pltpu.SemaphoreType.DMA((6,)),
            pltpu.SemaphoreType.DMA((6,)),
        ],
        compiler_params=pltpu.CompilerParams(
            collective_id=0, has_side_effects=True, vmem_limit_bytes=50 * 2**20
        ),
        name="cahn_hilliard_step",
    )(
        concentration.reshape(ROWS * COLS, NZ),
        jnp.asarray(tables),
    )
    updated, mass = pl.pallas_call(
        deliver,
        out_shape=(
            jax.ShapeDtypeStruct((ROWS * COLS, NZ), f32),
            jax.ShapeDtypeStruct((1, 1), f32),
        ),
        in_specs=[vmem, vmem],
        out_specs=(anywhere, vmem),
        scratch_shapes=[pltpu.SemaphoreType.DMA((2, 4))],
        compiler_params=pltpu.CompilerParams(vmem_limit_bytes=8 * 2**20),
        name="deliver",
    )(halves, mass)
    return updated.reshape(ROWS, COLS, NZ), mass.reshape(())


def solution(mesh):
    return jax.shard_map(
        local,
        mesh=mesh,
        in_specs=(P("slab", "pencil", None),),
        out_specs=(P("slab", "pencil", None), P()),
        check_vma=False,
    )
```

```python
import functools
import math

import jax
import jax.numpy as jnp
import numpy as np
from jax import lax
from jax.experimental import pallas as pl
from jax.experimental.pallas import tpu as pltpu
from jax.sharding import PartitionSpec as P

NX = 512
NY = 512
NZ = 256
KEPT = NZ // 2
DEVICES = 128
ROWS = 256
COLS = 8
HALF = ROWS // 2
TOTAL = NX * NY * NZ
NEAR_LAST = [22, 23, 13, 14, 15, 26, 6, 17, 18, 29, 19, 30, 20, 31, 10, 21, 11, 12, 2, 25, 5, 16, 27, 28, 7, 9, 1, 24, 3, 4, 8]
FIRST = 0

time_step = 1.0
stiffness = 1.0

MESH = pl.DeviceIdType.MESH
f32 = jnp.float32
bf16 = jnp.bfloat16


def all_tables():
    full = np.concatenate([depth_tables(), *plane_tables()])
    high = full.astype(np.float32).astype(bf16)
    low = (full - high.astype(np.float64)).astype(np.float32).astype(bf16)
    return np.stack([high, low], axis=1).reshape(20, 256, 256)


def depth_tables():
    k = np.arange(KEPT)[:, None]
    n = np.arange(NZ)[None, :]
    angle = 2.0 * np.pi * (k * n % NZ) / NZ
    forward = np.concatenate([np.cos(angle), -np.sin(angle)], axis=0)
    weight = np.where(k == 0, 1.0, 2.0) / TOTAL
    inverse = np.stack([weight * np.cos(angle), -weight * np.sin(angle)], axis=1)
    return forward, inverse.reshape(NZ, NZ)


def plane_tables():
    c = np.arange(128)[:, None]
    b = np.arange(128)[None, :]
    out = []
    for d in range(4):
        angle = 2.0 * np.pi * (b * (4 * c + d) % 512) / 512
        cos, sin = np.cos(angle), np.sin(angle)
        out.append(np.block([[cos, sin], [-sin, cos]]))
    full = np.stack(out)
    return full, full.transpose(0, 2, 1)


def parts(value):
    high = value.astype(bf16)
    return high, (value - high.astype(f32)).astype(bf16)


def product(left, right, dims):
    dot = functools.partial(
        lax.dot_general, dimension_numbers=(dims, ((), ())), preferred_element_type=f32
    )
    return dot(left[0], right[0]) + (dot(left[0], right[1]) + dot(left[1], right[0]))


def spread(xr, xi):
    sr, si = xr[0] + xr[2], xi[0] + xi[2]
    tr, ti = xr[1] + xr[3], xi[1] + xi[3]
    pr, pi = xr[0] - xr[2], xi[0] - xi[2]
    qr, qi = xr[1] - xr[3], xi[1] - xi[3]
    return (
        (sr + tr, si + ti),
        (pr + qi, pi - qr),
        (sr - tr, si - ti),
        (pr - qi, pi + qr),
    )


def gather(vr, vi):
    sr, si = vr[0] + vr[2], vi[0] + vi[2]
    tr, ti = vr[1] + vr[3], vi[1] + vi[3]
    pr, pi = vr[0] - vr[2], vi[0] - vi[2]
    qr, qi = vr[1] - vr[3], vi[1] - vi[3]
    return (
        (sr + tr, si + ti),
        (pr - qi, pi + qr),
        (sr - tr, si - ti),
        (pr + qi, pi - qr),
    )


def wave(index):
    signed = jnp.where(index < 256, index, index - 512)
    return (2.0 * math.pi / 512) * signed.astype(f32)


def kernel(
    conc_hbm, tables_hbm,
    out, mass_ref,
    conc, tables, send_c, send_q, plane, back, got, retain, forcing,
    load_sem, local_sem, send_sem, recv_sem,
):
    slab = lax.axis_index("slab")
    pencil = lax.axis_index("pencil")
    me = slab * 64 + pencil

    barrier = pltpu.get_barrier_semaphore()

    def greet(step, carry):
        to = lax.rem(me + step, DEVICES)
        pl.semaphore_signal(
            barrier,
            inc=1,
            device_id=(lax.div(to, 64), lax.rem(to, 64)),
            device_id_type=MESH,
        )
        return carry

    loads = [
        pltpu.make_async_copy(src, dst, load_sem.at[i])
        for i, (src, dst) in enumerate(
            [
                (conc_hbm.at[:, 0:128], conc.at[0]),
                (conc_hbm.at[:, 128:256], conc.at[1]),
                (tables_hbm.at[0:2], tables.at[0:2]),
                (tables_hbm.at[2:20], tables.at[2:20]),
            ]
        )
    ]
    for load in loads:
        load.start()
    lax.fori_loop(1, DEVICES, greet, 0)
    for load in loads[:3]:
        load.wait()

    def table(first):
        return tables[first], tables[first + 1]

    def forward_table(d):
        return table(4 + 2 * d)

    def turned_table(d):
        return table(12 + 2 * d)

    def depth_forward(cubed, sends, h):
        def body(j, carry):
            value = jnp.concatenate(
                [
                    jnp.concatenate(
                        [
                            conc[i, pl.ds(h * HALF * COLS + 2 * j + e, HALF, stride=COLS), :]
                            for i in range(2)
                        ],
                        axis=1,
                    )
                    for e in range(2)
                ],
                axis=0,
            )
            if cubed:
                value = value * value * value
            result = product(table(0), parts(value), ((1,), (1,)))
            for i in range(2):
                for e in range(2):
                    sends[h, pl.ds(i * COLS + 2 * j + e, KEPT, stride=2 * COLS), :] = result[
                        i * KEPT : (i + 1) * KEPT, e * HALF : (e + 1) * HALF
                    ]
            return carry

        lax.fori_loop(0, COLS // 2, body, 0, unroll=True)

    def forward_block(sends, field, h, to_slab, to_pencil):
        return (
            sends.at[
                h, pl.ds(pl.multiple_of(to_slab * 1024 + to_pencil * 16, 16), 16), :
            ].reshape(2, 8, 128),
            plane.at[
                2 * field : 2 * field + 2,
                pl.ds(pl.multiple_of(pencil * COLS, COLS), COLS),
                pl.ds(pl.multiple_of(slab * ROWS + h * HALF, HALF), HALF),
            ],
        )

    def backward_block(h, to_slab, to_pencil):
        return (
            back.at[
                :,
                pl.ds(pl.multiple_of(to_pencil * COLS, COLS), COLS),
                pl.ds(pl.multiple_of(to_slab * ROWS + h * HALF, HALF), HALF),
            ],
            got.at[h, pl.ds(pl.multiple_of(me * 16, 16), 16), :].reshape(2, 8, 128),
        )

    def keep_own(block, stage):
        src, dst = block(slab, pencil)
        pltpu.make_async_copy(src, dst, local_sem.at[stage]).start()

    def exchange(block, stage, core):
        def send(to_slab, to_pencil):
            src, dst = block(to_slab, to_pencil)
            pltpu.make_async_remote_copy(
                src_ref=src,
                dst_ref=dst,
                send_sem=send_sem.at[stage],
                recv_sem=recv_sem.at[stage],
                device_id=(to_slab, to_pencil),
                device_id_type=MESH,
            ).start()

        chip = lax.div(pencil, 2)

        def pair(turn, carry):
            to_pencil = 2 * lax.rem(chip + 11 * turn, 32) + core
            send(slab, to_pencil)
            send(1 - slab, to_pencil)
            return carry

        if stage < 4:
            lax.fori_loop(1, 32, pair, 0)
        else:
            for turn in NEAR_LAST:
                to_pencil = 2 * lax.rem(chip + turn, 32) + core
                send(1 - slab, to_pencil)
                send(slab, to_pencil)
        send(1 - slab, 2 * chip + core)

        @pl.when(lax.rem(pencil, 2) != core)
        def _():
            send(slab, 2 * chip + core)

    def everything(stage):
        rows = pl.ds(0, 16 * (DEVICES - 1))
        return pltpu.make_async_remote_copy(
            src_ref=got.at[0, rows, :],
            dst_ref=got.at[0, rows, :],
            send_sem=send_sem.at[stage],
            recv_sem=recv_sem.at[stage],
            device_id=(slab, pencil),
            device_id_type=MESH,
        )

    def arrived(block, stage):
        src, dst = block(slab, pencil)
        pltpu.make_async_copy(src, dst, local_sem.at[stage]).wait()
        everything(stage).wait_recv()

    def lane_halves(h):
        return [slice(i * ROWS + h * HALF, i * ROWS + (h + 1) * HALF) for i in range(2)]

    def both(index, rows, h):
        return jnp.concatenate([plane[index, rows, lanes] for lanes in lane_halves(h)], axis=1)

    def second_forward(field, h):
        quarters = [slice(a * 128, (a + 1) * 128) for a in range(4)]
        xr = [both(2 * field, rows, h) for rows in quarters]
        xi = [both(2 * field + 1, rows, h) for rows in quarters]
        for d, (ur, ui) in enumerate(spread(xr, xi)):
            result = product(
                forward_table(d), parts(jnp.concatenate([ur, ui], axis=0)), ((1,), (0,))
            )
            for i, lanes in enumerate(lane_halves(h)):
                half = slice(i * HALF, (i + 1) * HALF)
                plane[2 * field, quarters[d], lanes] = result[:128, half]
                plane[2 * field + 1, quarters[d], lanes] = result[128:, half]

    def first_forward(field, rows):
        xr = [plane[2 * field, rows, a * 128 : (a + 1) * 128] for a in range(4)]
        xi = [plane[2 * field + 1, rows, a * 128 : (a + 1) * 128] for a in range(4)]
        return [
            product(parts(jnp.concatenate([ur, ui], axis=1)), turned_table(d), ((1,), (0,)))
            for d, (ur, ui) in enumerate(spread(xr, xi))
        ]

    def row_block(i):
        return pl.ds(pl.multiple_of(i * 128, 128), 128)

    def first_forward_conc():
        def body(i, carry):
            rows = row_block(i)
            for d, result in enumerate(first_forward(0, rows)):
                plane[0, rows, d * 128 : (d + 1) * 128] = result[:, :128]
                plane[1, rows, d * 128 : (d + 1) * 128] = result[:, 128:]
            return carry

        lax.fori_loop(0, 4, body, 0)

    def multipliers():
        third = wave(me) * (512 // NZ)

        def body(i, carry):
            rows = row_block(i)
            row = lax.broadcasted_iota(jnp.int32, (128, 512), 0)
            lane = lax.broadcasted_iota(jnp.int32, (128, 512), 1)
            second = wave(row * 4 + i)
            first = wave(lane % 128 * 4 + lane // 128)
            square = first * first + second * second + third * third
            divisor = 1.0 + time_step * stiffness * square * square
            retain[rows, :] = (1.0 + time_step * square) / divisor
            forcing[rows, :] = (time_step * square) / divisor
            return carry

        lax.fori_loop(0, 4, body, 0)

    def combine_and_first_inverse():
        def body(i, carry):
            rows = row_block(i)
            vr, vi = [], []
            for d, cube in enumerate(first_forward(1, rows)):
                lanes = slice(d * 128, (d + 1) * 128)
                keep, force = retain[rows, lanes], forcing[rows, lanes]
                next_real = keep * plane[0, rows, lanes] - force * cube[:, :128]
                next_imag = keep * plane[1, rows, lanes] - force * cube[:, 128:]
                result = product(
                    parts(jnp.concatenate([next_real, next_imag], axis=1)),
                    forward_table(d),
                    ((1,), (0,)),
                )
                vr.append(result[:, :128])
                vi.append(result[:, 128:])
            for a, (xr, xi) in enumerate(gather(vr, vi)):
                plane[2, rows, a * 128 : (a + 1) * 128] = xr
                plane[3, rows, a * 128 : (a + 1) * 128] = xi
            return carry

        lax.fori_loop(0, 4, body, 0)

    def second_inverse(h, mass):
        quarters = [slice(a * 128, (a + 1) * 128) for a in range(4)]
        vr, vi = [], []
        for d in range(4):
            value = jnp.concatenate([both(2, quarters[d], h), both(3, quarters[d], h)], axis=0)
            result = product(turned_table(d), parts(value), ((1,), (0,)))
            vr.append(result[:128])
            vi.append(result[128:])
        for a, (xr, xi) in enumerate(gather(vr, vi)):
            xi = jnp.where(me == 0, mass, xi)
            for i, lanes in enumerate(lane_halves(h)):
                half = slice(i * HALF, (i + 1) * HALF)
                back[0, quarters[a], lanes] = xr[:, half]
                back[1, quarters[a], lanes] = xi[:, half]

    def depth_inverse(h):
        def body(j, carry):
            value = jnp.concatenate(
                [got[h, pl.ds(2 * j + e, NZ, stride=COLS), :] for e in range(2)], axis=1
            )
            result = product(parts(value), table(2), ((0,), (0,)))
            for e in range(2):
                for i in range(2):
                    out[i, pl.ds(h * HALF * COLS + 2 * j + e, HALF, stride=COLS), :] = result[
                        e * HALF : (e + 1) * HALF, i * 128 : (i + 1) * 128
                    ]
            return carry

        lax.fori_loop(0, COLS // 2, body, 0, unroll=True)

    def forward_stage(stage):
        sends = send_c if stage < 2 else send_q
        return functools.partial(forward_block, sends, stage // 2, stage % 2)

    for stage in range(4):
        depth_forward(stage >= 2, send_c if stage < 2 else send_q, stage % 2)
        if stage == 0:
            pl.semaphore_wait(barrier, DEVICES - 1)
        keep_own(forward_stage(stage), stage)
        exchange(forward_stage(stage), stage, FIRST)
    for stage in range(4):
        exchange(forward_stage(stage), stage, 1 - FIRST)
    multipliers()
    loads[3].wait()
    for h in range(2):
        arrived(forward_stage(h), h)
        second_forward(0, h)
    first_forward_conc()
    mass = jnp.broadcast_to(plane[0, 0:1, 0:1], (128, 256)) * (1.0 / TOTAL)
    for h in range(2):
        arrived(forward_stage(2 + h), 2 + h)
        second_forward(1, h)
    combine_and_first_inverse()
    for h in range(2):
        block = functools.partial(backward_block, h)
        second_inverse(h, mass)
        keep_own(block, 4 + h)
        exchange(block, 4 + h, 1)
        exchange(block, 4 + h, 0)
    for h in range(2):
        arrived(functools.partial(backward_block, h), 4 + h)
        depth_inverse(h)
    mass_ref[...] = got[0, 8:16, :]
    for stage in range(6):
        everything(stage).wait_send()


def deliver(parts_ref, mass_in, out_hbm, mass_ref, sem):
    copies = [
        pltpu.make_async_copy(
            parts_ref.at[i, r * 512 : (r + 1) * 512, :],
            out_hbm.at[r * 512 : (r + 1) * 512, i * 128 : (i + 1) * 128],
            sem.at[i, r],
        )
        for r in range(4)
        for i in range(2)
    ]
    for copy in copies:
        copy.start()
    mass_ref[...] = mass_in[0:1, 0:1]
    for copy in copies:
        copy.wait()


def local(concentration):
    tables = all_tables()
    anywhere = pl.BlockSpec(memory_space=pl.ANY)
    vmem = pl.BlockSpec(memory_space=pltpu.VMEM)
    halves, mass = pl.pallas_call(
        kernel,
        out_shape=(
            jax.ShapeDtypeStruct((2, ROWS * COLS, 128), f32),
            jax.ShapeDtypeStruct((8, 128), f32),
        ),
        in_specs=[anywhere] * 2,
        out_specs=(vmem, vmem),
        scratch_shapes=[
            pltpu.VMEM((2, ROWS * COLS, 128), f32),
            pltpu.VMEM(tables.shape, bf16),
            pltpu.VMEM((2, KEPT * 16, HALF), f32),
            pltpu.VMEM((2, KEPT * 16, HALF), f32),
            pltpu.VMEM((4, NY, NX), f32),
            pltpu.VMEM((2, NY, NX), f32),
            pltpu.VMEM((2, KEPT * 16, HALF), f32),
            pltpu.VMEM((NY, NX), f32),
            pltpu.VMEM((NY, NX), f32),
            pltpu.SemaphoreType.DMA((4,)),
            pltpu.SemaphoreType.DMA((6,)),
            pltpu.SemaphoreType.DMA((6,)),
            pltpu.SemaphoreType.DMA((6,)),
        ],
        compiler_params=pltpu.CompilerParams(
            collective_id=0, has_side_effects=True, vmem_limit_bytes=50 * 2**20
        ),
        name="cahn_hilliard_step",
    )(
        concentration.reshape(ROWS * COLS, NZ),
        jnp.asarray(tables),
    )
    updated, mass = pl.pallas_call(
        deliver,
        out_shape=(
            jax.ShapeDtypeStruct((ROWS * COLS, NZ), f32),
            jax.ShapeDtypeStruct((1, 1), f32),
        ),
        in_specs=[vmem, vmem],
        out_specs=(anywhere, vmem),
        scratch_shapes=[pltpu.SemaphoreType.DMA((2, 4))],
        compiler_params=pltpu.CompilerParams(vmem_limit_bytes=8 * 2**20),
        name="deliver",
    )(halves, mass)
    return updated.reshape(ROWS, COLS, NZ), mass.reshape(())


def solution(mesh):
    return jax.shard_map(
        local,
        mesh=mesh,
        in_specs=(P("slab", "pencil", None),),
        out_specs=(P("slab", "pencil", None), P()),
        check_vma=False,
    )
```

```python
import functools
import math

import jax
import jax.numpy as jnp
import numpy as np
from jax import lax
from jax.experimental import pallas as pl
from jax.experimental.pallas import tpu as pltpu
from jax.sharding import PartitionSpec as P

NX = 512
NY = 512
NZ = 256
KEPT = NZ // 2
DEVICES = 128
ROWS = 256
COLS = 8
HALF = ROWS // 2
TOTAL = NX * NY * NZ
NEAR_LAST = [22, 23, 13, 14, 15, 26, 6, 17, 18, 29, 19, 30, 20, 31, 10, 21, 11, 12, 2, 25, 5, 16, 27, 28, 7, 9, 1, 24, 3, 4, 8]
FIRST = 0

time_step = 1.0
stiffness = 1.0

MESH = pl.DeviceIdType.MESH
f32 = jnp.float32
bf16 = jnp.bfloat16


def all_tables():
    full = np.concatenate([depth_tables(), *plane_tables()])
    high = full.astype(np.float32).astype(bf16)
    low = (full - high.astype(np.float64)).astype(np.float32).astype(bf16)
    return np.stack([high, low], axis=1).reshape(20, 256, 256)


def depth_tables():
    k = np.arange(KEPT)[:, None]
    n = np.arange(NZ)[None, :]
    angle = 2.0 * np.pi * (k * n % NZ) / NZ
    forward = np.concatenate([np.cos(angle), -np.sin(angle)], axis=0)
    weight = np.where(k == 0, 1.0, 2.0) / TOTAL
    inverse = np.stack([weight * np.cos(angle), -weight * np.sin(angle)], axis=1)
    return forward, inverse.reshape(NZ, NZ)


def plane_tables():
    c = np.arange(128)[:, None]
    b = np.arange(128)[None, :]
    out = []
    for d in range(4):
        angle = 2.0 * np.pi * (b * (4 * c + d) % 512) / 512
        cos, sin = np.cos(angle), np.sin(angle)
        out.append(np.block([[cos, sin], [-sin, cos]]))
    full = np.stack(out)
    return full, full.transpose(0, 2, 1)


def parts(value):
    high = value.astype(bf16)
    return high, (value - high.astype(f32)).astype(bf16)


def product(left, right, dims):
    dot = functools.partial(
        lax.dot_general, dimension_numbers=(dims, ((), ())), preferred_element_type=f32
    )
    return dot(left[0], right[0]) + (dot(left[0], right[1]) + dot(left[1], right[0]))


def spread(xr, xi):
    sr, si = xr[0] + xr[2], xi[0] + xi[2]
    tr, ti = xr[1] + xr[3], xi[1] + xi[3]
    pr, pi = xr[0] - xr[2], xi[0] - xi[2]
    qr, qi = xr[1] - xr[3], xi[1] - xi[3]
    return (
        (sr + tr, si + ti),
        (pr + qi, pi - qr),
        (sr - tr, si - ti),
        (pr - qi, pi + qr),
    )


def gather(vr, vi):
    sr, si = vr[0] + vr[2], vi[0] + vi[2]
    tr, ti = vr[1] + vr[3], vi[1] + vi[3]
    pr, pi = vr[0] - vr[2], vi[0] - vi[2]
    qr, qi = vr[1] - vr[3], vi[1] - vi[3]
    return (
        (sr + tr, si + ti),
        (pr - qi, pi + qr),
        (sr - tr, si - ti),
        (pr + qi, pi - qr),
    )


def wave(index):
    signed = jnp.where(index < 256, index, index - 512)
    return (2.0 * math.pi / 512) * signed.astype(f32)


def kernel(
    conc_hbm, tables_hbm,
    out, mass_ref,
    conc, tables, send_c, send_q, plane, back, got, retain, forcing,
    load_sem, local_sem, send_sem, recv_sem,
):
    slab = lax.axis_index("slab")
    pencil = lax.axis_index("pencil")
    me = slab * 64 + pencil

    barrier = pltpu.get_barrier_semaphore()

    def greet(step, carry):
        to = lax.rem(me + step, DEVICES)
        pl.semaphore_signal(
            barrier,
            inc=1,
            device_id=(lax.div(to, 64), lax.rem(to, 64)),
            device_id_type=MESH,
        )
        return carry

    loads = [
        pltpu.make_async_copy(src, dst, load_sem.at[i])
        for i, (src, dst) in enumerate(
            [
                (conc_hbm.at[:, 0:128], conc.at[0]),
                (conc_hbm.at[:, 128:256], conc.at[1]),
                (tables_hbm.at[0:2], tables.at[0:2]),
                (tables_hbm.at[2:20], tables.at[2:20]),
            ]
        )
    ]
    for load in loads:
        load.start()
    lax.fori_loop(1, DEVICES, greet, 0)
    for load in loads[:3]:
        load.wait()

    def table(first):
        return tables[first], tables[first + 1]

    def forward_table(d):
        return table(4 + 2 * d)

    def turned_table(d):
        return table(12 + 2 * d)

    def depth_forward(cubed, sends, h):
        def body(j, carry):
            value = jnp.concatenate(
                [
                    jnp.concatenate(
                        [
                            conc[i, pl.ds(h * HALF * COLS + 2 * j + e, HALF, stride=COLS), :]
                            for i in range(2)
                        ],
                        axis=1,
                    )
                    for e in range(2)
                ],
                axis=0,
            )
            if cubed:
                value = value * value * value
            result = product(table(0), parts(value), ((1,), (1,)))
            for i in range(2):
                for e in range(2):
                    sends[h, pl.ds(i * COLS + 2 * j + e, KEPT, stride=2 * COLS), :] = result[
                        i * KEPT : (i + 1) * KEPT, e * HALF : (e + 1) * HALF
                    ]
            return carry

        lax.fori_loop(0, COLS // 2, body, 0, unroll=True)

    def forward_block(sends, field, h, to_slab, to_pencil):
        return (
            sends.at[
                h, pl.ds(pl.multiple_of(to_slab * 1024 + to_pencil * 16, 16), 16), :
            ].reshape(2, 8, 128),
            plane.at[
                2 * field : 2 * field + 2,
                pl.ds(pl.multiple_of(pencil * COLS, COLS), COLS),
                pl.ds(pl.multiple_of(slab * ROWS + h * HALF, HALF), HALF),
            ],
        )

    def backward_block(h, to_slab, to_pencil):
        return (
            back.at[
                :,
                pl.ds(pl.multiple_of(to_pencil * COLS, COLS), COLS),
                pl.ds(pl.multiple_of(to_slab * ROWS + h * HALF, HALF), HALF),
            ],
            got.at[h, pl.ds(pl.multiple_of(me * 16, 16), 16), :].reshape(2, 8, 128),
        )

    def keep_own(block, stage):
        src, dst = block(slab, pencil)
        pltpu.make_async_copy(src, dst, local_sem.at[stage]).start()

    def exchange(block, stage, core):
        def send(to_slab, to_pencil):
            src, dst = block(to_slab, to_pencil)
            pltpu.make_async_remote_copy(
                src_ref=src,
                dst_ref=dst,
                send_sem=send_sem.at[stage],
                recv_sem=recv_sem.at[stage],
                device_id=(to_slab, to_pencil),
                device_id_type=MESH,
            ).start()

        chip = lax.div(pencil, 2)

        def pair(turn, carry):
            to_pencil = 2 * lax.rem(chip + 11 * turn, 32) + core
            send(slab, to_pencil)
            send(1 - slab, to_pencil)
            return carry

        if stage < 4:
            lax.fori_loop(1, 32, pair, 0)
        else:
            for turn in NEAR_LAST:
                to_pencil = 2 * lax.rem(chip + turn, 32) + core
                send(1 - slab, to_pencil)
                send(slab, to_pencil)
        send(1 - slab, 2 * chip + core)

        @pl.when(lax.rem(pencil, 2) != core)
        def _():
            send(slab, 2 * chip + core)

    def everything(stage):
        rows = pl.ds(0, 16 * (DEVICES - 1))
        return pltpu.make_async_remote_copy(
            src_ref=got.at[0, rows, :],
            dst_ref=got.at[0, rows, :],
            send_sem=send_sem.at[stage],
            recv_sem=recv_sem.at[stage],
            device_id=(slab, pencil),
            device_id_type=MESH,
        )

    def arrived(block, stage):
        src, dst = block(slab, pencil)
        pltpu.make_async_copy(src, dst, local_sem.at[stage]).wait()
        everything(stage).wait_recv()

    def lane_halves(h):
        return [slice(i * ROWS + h * HALF, i * ROWS + (h + 1) * HALF) for i in range(2)]

    def both(index, rows, h):
        return jnp.concatenate([plane[index, rows, lanes] for lanes in lane_halves(h)], axis=1)

    def second_forward(field, h):
        quarters = [slice(a * 128, (a + 1) * 128) for a in range(4)]
        xr = [both(2 * field, rows, h) for rows in quarters]
        xi = [both(2 * field + 1, rows, h) for rows in quarters]
        for d, (ur, ui) in enumerate(spread(xr, xi)):
            result = product(
                forward_table(d), parts(jnp.concatenate([ur, ui], axis=0)), ((1,), (0,))
            )
            for i, lanes in enumerate(lane_halves(h)):
                half = slice(i * HALF, (i + 1) * HALF)
                plane[2 * field, quarters[d], lanes] = result[:128, half]
                plane[2 * field + 1, quarters[d], lanes] = result[128:, half]

    def first_forward(field, rows):
        xr = [plane[2 * field, rows, a * 128 : (a + 1) * 128] for a in range(4)]
        xi = [plane[2 * field + 1, rows, a * 128 : (a + 1) * 128] for a in range(4)]
        return [
            product(parts(jnp.concatenate([ur, ui], axis=1)), turned_table(d), ((1,), (0,)))
            for d, (ur, ui) in enumerate(spread(xr, xi))
        ]

    def row_block(i):
        return pl.ds(pl.multiple_of(i * 128, 128), 128)

    def first_forward_conc():
        def body(i, carry):
            rows = row_block(i)
            for d, result in enumerate(first_forward(0, rows)):
                plane[0, rows, d * 128 : (d + 1) * 128] = result[:, :128]
                plane[1, rows, d * 128 : (d + 1) * 128] = result[:, 128:]
            return carry

        lax.fori_loop(0, 4, body, 0)

    def multipliers():
        third = wave(me) * (512 // NZ)

        def body(i, carry):
            rows = row_block(i)
            row = lax.broadcasted_iota(jnp.int32, (128, 512), 0)
            lane = lax.broadcasted_iota(jnp.int32, (128, 512), 1)
            second = wave(row * 4 + i)
            first = wave(lane % 128 * 4 + lane // 128)
            square = first * first + second * second + third * third
            divisor = 1.0 + time_step * stiffness * square * square
            retain[rows, :] = (1.0 + time_step * square) / divisor
            forcing[rows, :] = (time_step * square) / divisor
            return carry

        lax.fori_loop(0, 4, body, 0)

    def combine_and_first_inverse():
        def body(i, carry):
            rows = pl.ds(pl.multiple_of(i * 256, 256), 256)
            vr, vi = [], []
            for d, cube in enumerate(first_forward(1, rows)):
                lanes = slice(d * 128, (d + 1) * 128)
                keep, force = retain[rows, lanes], forcing[rows, lanes]
                next_real = keep * plane[0, rows, lanes] - force * cube[:, :128]
                next_imag = keep * plane[1, rows, lanes] - force * cube[:, 128:]
                result = product(
                    parts(jnp.concatenate([next_real, next_imag], axis=1)),
                    forward_table(d),
                    ((1,), (0,)),
                )
                vr.append(result[:, :128])
                vi.append(result[:, 128:])
            for a, (xr, xi) in enumerate(gather(vr, vi)):
                plane[2, rows, a * 128 : (a + 1) * 128] = xr
                plane[3, rows, a * 128 : (a + 1) * 128] = xi
            return carry

        lax.fori_loop(0, 2, body, 0)

    def second_inverse(h, mass):
        quarters = [slice(a * 128, (a + 1) * 128) for a in range(4)]
        vr, vi = [], []
        for d in range(4):
            value = jnp.concatenate([both(2, quarters[d], h), both(3, quarters[d], h)], axis=0)
            result = product(turned_table(d), parts(value), ((1,), (0,)))
            vr.append(result[:128])
            vi.append(result[128:])
        for a, (xr, xi) in enumerate(gather(vr, vi)):
            xi = jnp.where(me == 0, mass, xi)
            for i, lanes in enumerate(lane_halves(h)):
                half = slice(i * HALF, (i + 1) * HALF)
                back[0, quarters[a], lanes] = xr[:, half]
                back[1, quarters[a], lanes] = xi[:, half]

    def depth_inverse(h):
        def body(j, carry):
            value = jnp.concatenate(
                [got[h, pl.ds(2 * j + e, NZ, stride=COLS), :] for e in range(2)], axis=1
            )
            result = product(parts(value), table(2), ((0,), (0,)))
            for e in range(2):
                for i in range(2):
                    out[i, pl.ds(h * HALF * COLS + 2 * j + e, HALF, stride=COLS), :] = result[
                        e * HALF : (e + 1) * HALF, i * 128 : (i + 1) * 128
                    ]
            return carry

        lax.fori_loop(0, COLS // 2, body, 0, unroll=True)

    def forward_stage(stage):
        sends = send_c if stage < 2 else send_q
        return functools.partial(forward_block, sends, stage // 2, stage % 2)

    for stage in range(4):
        depth_forward(stage >= 2, send_c if stage < 2 else send_q, stage % 2)
        if stage == 0:
            pl.semaphore_wait(barrier, DEVICES - 1)
        keep_own(forward_stage(stage), stage)
        exchange(forward_stage(stage), stage, FIRST)
    for stage in range(4):
        exchange(forward_stage(stage), stage, 1 - FIRST)
    multipliers()
    loads[3].wait()
    for h in range(2):
        arrived(forward_stage(h), h)
        second_forward(0, h)
    first_forward_conc()
    mass = jnp.broadcast_to(plane[0, 0:1, 0:1], (128, 256)) * (1.0 / TOTAL)
    for h in range(2):
        arrived(forward_stage(2 + h), 2 + h)
        second_forward(1, h)
    combine_and_first_inverse()
    for h in range(2):
        block = functools.partial(backward_block, h)
        second_inverse(h, mass)
        keep_own(block, 4 + h)
        exchange(block, 4 + h, 1)
        exchange(block, 4 + h, 0)
    for h in range(2):
        arrived(functools.partial(backward_block, h), 4 + h)
        depth_inverse(h)
    mass_ref[...] = got[0, 8:16, :]
    for stage in range(6):
        everything(stage).wait_send()


def deliver(parts_ref, mass_in, out_hbm, mass_ref, sem):
    copies = [
        pltpu.make_async_copy(
            parts_ref.at[i, r * 512 : (r + 1) * 512, :],
            out_hbm.at[r * 512 : (r + 1) * 512, i * 128 : (i + 1) * 128],
            sem.at[i, r],
        )
        for r in range(4)
        for i in range(2)
    ]
    for copy in copies:
        copy.start()
    mass_ref[...] = mass_in[0:1, 0:1]
    for copy in copies:
        copy.wait()


def local(concentration):
    tables = all_tables()
    anywhere = pl.BlockSpec(memory_space=pl.ANY)
    vmem = pl.BlockSpec(memory_space=pltpu.VMEM)
    halves, mass = pl.pallas_call(
        kernel,
        out_shape=(
            jax.ShapeDtypeStruct((2, ROWS * COLS, 128), f32),
            jax.ShapeDtypeStruct((8, 128), f32),
        ),
        in_specs=[anywhere] * 2,
        out_specs=(vmem, vmem),
        scratch_shapes=[
            pltpu.VMEM((2, ROWS * COLS, 128), f32),
            pltpu.VMEM(tables.shape, bf16),
            pltpu.VMEM((2, KEPT * 16, HALF), f32),
            pltpu.VMEM((2, KEPT * 16, HALF), f32),
            pltpu.VMEM((4, NY, NX), f32),
            pltpu.VMEM((2, NY, NX), f32),
            pltpu.VMEM((2, KEPT * 16, HALF), f32),
            pltpu.VMEM((NY, NX), f32),
            pltpu.VMEM((NY, NX), f32),
            pltpu.SemaphoreType.DMA((4,)),
            pltpu.SemaphoreType.DMA((6,)),
            pltpu.SemaphoreType.DMA((6,)),
            pltpu.SemaphoreType.DMA((6,)),
        ],
        compiler_params=pltpu.CompilerParams(
            collective_id=0, has_side_effects=True, vmem_limit_bytes=50 * 2**20
        ),
        name="cahn_hilliard_step",
    )(
        concentration.reshape(ROWS * COLS, NZ),
        jnp.asarray(tables),
    )
    updated, mass = pl.pallas_call(
        deliver,
        out_shape=(
            jax.ShapeDtypeStruct((ROWS * COLS, NZ), f32),
            jax.ShapeDtypeStruct((1, 1), f32),
        ),
        in_specs=[vmem, vmem],
        out_specs=(anywhere, vmem),
        scratch_shapes=[pltpu.SemaphoreType.DMA((2, 4))],
        compiler_params=pltpu.CompilerParams(vmem_limit_bytes=8 * 2**20),
        name="deliver",
    )(halves, mass)
    return updated.reshape(ROWS, COLS, NZ), mass.reshape(())


def solution(mesh):
    return jax.shard_map(
        local,
        mesh=mesh,
        in_specs=(P("slab", "pencil", None),),
        out_specs=(P("slab", "pencil", None), P()),
        check_vma=False,
    )
```
